32 devices in a mesh: slab: 4 (over z), sub: 8 (over y, x, core).
Axes of the slice: x: 2, y: 2, z: 4, core: 2. Of those that a mesh axis runs over, the one named last changes fastest.
Arguments:
- near_null: float32 [18, 16384], P(None, ('slab', 'sub')), may hold values from -48 to 48
- aggregates: int32 [16384], P(('slab', 'sub')), may hold values from 0 to 63
- diag_block: float32 [9, 16384], P(None, ('slab', 'sub')), may hold values from -1 to 12, as said below
- off_blocks: float32 [26, 9, 16384], P(None, None, ('slab', 'sub')), may hold values from -18 to 18
- columns: int32 [26, 16384], P(None, ('slab', 'sub')), may hold values from 0 to 767, as said below
- sends: int32 [4, 2048], P(None, ('slab', 'sub')), may hold values from 0 to 511
- start_vector: float32 [3, 16384], P(None, ('slab', 'sub')), may hold values from -18 to 18
Outputs:
- prolong_off: bfloat16 [26, 18, 16384], P(None, None, ('slab', 'sub'))
- prolong_self: bfloat16 [18, 16384], P(None, ('slab', 'sub'))
- rho: float32 [], replicated
The draws below stay inside these ranges and needn't reach their ends.
Inputs may be any that keep to these rules, and one draw needn't show every extreme that they name: `diag_block`: each block, read as 3x3 row-major, is symmetric with diagonal entries between 6 and 12 and off-diagonal entries between -1 and 1. `columns`: entries below 512 name a node of the same device; an entry c of 512 or more names ghost slot c - 512. Row e lists, for each device, the local rows it sends to its neighbour at sub + 1, sub - 1, slab + 1, slab - 1 for e = 0, 1, 2, 3. `aggregates`: aggregates lie within one device.
All inputs are finite; a program needn't handle non-finite values.
Results may differ from the reference program's by a relative error of at most 0.001.
Values sent between devices are 32-bit elements; how exact they have to be, the bound alone decides.
A program may use at most 64 MiB of HBM per device.

```python
import jax
import jax.numpy as jnp
from jax import lax

NB = 512
K = 26
ITERS = 8
GH = 64
AGG = 64
NODES = 16384
N_SLAB = 4
N_SUB = 8


def draw_diag_block(key, part):
    first_key, second_key = jax.random.split(key)
    middle = jax.random.uniform(first_key, (3, NODES), jnp.float32, 6.0, 12.0)
    side = jax.random.uniform(second_key, (3, NODES), jnp.float32, -1.0, 1.0)
    return jnp.stack([middle[0], side[0], side[1], side[0], middle[1], side[2], side[1], side[2], middle[2]])


def draw_start_vector(key, part):
    owner = (jnp.arange(NODES, dtype=jnp.int32) // NB).astype(jnp.float32)
    last_device = float(max(NODES // NB - 1, 1))
    base = jnp.clip(jax.random.normal(key, (3, NODES), jnp.float32), -6.0, 6.0)
    scale = 3.0 ** (owner / last_device)
    return base * scale[None, :]


def draw_columns(key, part):
    local_key, remote_key, pick_key = jax.random.split(jax.random.fold_in(key, 17), 3)
    nearby = jax.random.randint(local_key, (K, NODES), 0, NB, jnp.int32)
    remote = jax.random.randint(remote_key, (K, NODES), NB, NB + 4 * GH, jnp.int32)
    chooser = jax.random.randint(pick_key, (K, NODES), 0, 100, jnp.int32)
    result = jnp.where(chooser < 15, remote, nearby).astype(jnp.int32)
    result = result.at[0, 0].set(0)
    result = result.at[1, 0].set(NB + 4 * GH - 1)
    return result


def with_ends(drawn, own_key, smallest, top_value):
    place = [jax.random.randint(jax.random.fold_in(own_key, axis), (), 0, length) for axis, length in enumerate(drawn.shape)]
    main_axis = drawn.shape.index(max(drawn.shape))
    next_to = place[:main_axis] + [(place[main_axis] + 1) % drawn.shape[main_axis]] + place[main_axis + 1:]
    return drawn.at[tuple(place)].set(smallest).at[tuple(next_to)].set(top_value)


def levels(own_key, shape, pieces, smallest, largest):
    factor_of, own = 1.0, jax.random.fold_in(own_key, 6)
    for dim, parts in pieces:
        steps = jnp.exp(jax.random.uniform(jax.random.fold_in(own, dim), (parts,), jnp.float32, smallest / len(pieces), largest / len(pieces)))
        factor_of = factor_of * jnp.repeat(steps, shape[dim] // parts).reshape([-1 if axis == dim else 1 for axis in range(len(shape))])
    return factor_of


def bell_draw(own_key, shape, width, most, cuts=(), held_as=jnp.bfloat16):
    drawn = width * jax.random.normal(own_key, shape, jnp.float32)
    if cuts:
        drawn = drawn * levels(own_key, shape, cuts, -0.22, 0.18)
    return jnp.clip(drawn, -most, most).astype(held_as)


def setup_inputs(seed: int = 0) -> dict:
    arg_keys = jax.random.split(jax.random.key(seed), 8)
    near_null = bell_draw(arg_keys[0], (18, NODES), 8.0, 48.0, ((1, 32),), jnp.float32)
    aggregates = with_ends(jax.random.randint(arg_keys[1], (NODES,), 0, AGG), jax.random.fold_in(arg_keys[1], 1), 0, AGG - 1).astype(jnp.int32)
    diag_block = draw_diag_block(jax.random.fold_in(arg_keys[7], 71), 0)
    off_blocks = bell_draw(arg_keys[3], (K, 9, NODES), 3.0, 18.0, ((2, 32),), jnp.float32)
    columns = draw_columns(jax.random.fold_in(arg_keys[7], 71), 0)
    sends = with_ends(jax.random.randint(arg_keys[5], (4, GH * N_SLAB * N_SUB), 0, NB), jax.random.fold_in(arg_keys[5], 1), 0, NB - 1).astype(jnp.int32)
    start_vector = draw_start_vector(jax.random.fold_in(arg_keys[7], 71), 0)
    return {"near_null": near_null, "aggregates": aggregates, "diag_block": diag_block, "off_blocks": off_blocks, "columns": columns, "sends": sends, "start_vector": start_vector}


OMEGA = 4.0 / 3.0
HIGHEST = lax.Precision.HIGHEST

def invert_blocks(diag_block):
    entries = [diag_block[position] for position in range(9)]
    cofactor = [entries[4] * entries[8] - entries[5] * entries[7], entries[5] * entries[6] - entries[3] * entries[8], entries[3] * entries[7] - entries[4] * entries[6], entries[2] * entries[7] - entries[1] * entries[8], entries[0] * entries[8] - entries[2] * entries[6], entries[1] * entries[6] - entries[0] * entries[7], entries[1] * entries[5] - entries[2] * entries[4], entries[2] * entries[3] - entries[0] * entries[5], entries[0] * entries[4] - entries[1] * entries[3]]
    determinant = entries[0] * cofactor[0] + entries[1] * cofactor[1] + entries[2] * cofactor[2]
    inverse = [cofactor[column * 3 + row_index] / determinant for row_index in range(3) for column in range(3)]
    return jnp.stack(inverse).reshape((3, 3) + diag_block.shape[1:])

def reference(near_null, aggregates, diag_block, off_blocks, columns, sends, start_vector):
    device_count = N_SLAB * N_SUB
    ghost_count = NB // 8
    group_count = NB // 8
    node_number = jnp.arange(NODES, dtype=jnp.int32)
    owner = (node_number // NB).astype(jnp.int32)
    segment = owner * group_count + aggregates
    counts = jax.ops.segment_sum(jnp.ones((NODES,), jnp.float32), segment, num_segments=device_count * group_count)
    tentative = near_null * lax.rsqrt(counts[segment])[None, :]
    inverse = invert_blocks(diag_block)
    device_number = jnp.arange(device_count, dtype=jnp.int32)
    slab_index = device_number // N_SUB
    sub_index = device_number % N_SUB
    neighbours = [(slab_index, sub_index - 1), (slab_index, sub_index + 1), (slab_index - 1, sub_index), (slab_index + 1, sub_index)]
    send_rows = sends.reshape(4, device_count, ghost_count)
    tables = []
    valids = []
    for direction in range(4):
        slab_pos, sub_pos = neighbours[direction]
        present = (slab_pos >= 0) & (slab_pos < N_SLAB) & (sub_pos >= 0) & (sub_pos < N_SUB)
        sender = (jnp.clip(slab_pos, 0, N_SLAB - 1) * N_SUB + jnp.clip(sub_pos, 0, N_SUB - 1)).astype(jnp.int32)
        tables.append(sender[:, None] * NB + send_rows[direction][sender])
        valids.append(jnp.broadcast_to(present[:, None], (device_count, ghost_count)))
    table = jnp.concatenate(tables, axis=1).reshape(-1).astype(jnp.int32)
    valid = jnp.concatenate(valids, axis=1).reshape(-1)
    inside = columns < NB
    remote_slot = jnp.clip(columns - NB, 0, 4 * ghost_count - 1)
    flat_slot = (owner[None, :] * (4 * ghost_count) + remote_slot).astype(jnp.int32)
    source = jnp.where(inside, owner[None, :] * NB + columns, table[flat_slot]).astype(jnp.int32)
    weight = jnp.where(inside, True, valid[flat_slot]).astype(jnp.float32)
    mats = off_blocks.reshape(off_blocks.shape[0], 3, 3, NODES)

    def operator(field):

        def add_slot(total, slot_data):
            block, anchor, scale = slot_data
            picked = field[:, anchor] * scale[None, :]
            return (total + jnp.einsum('rcn,cmn->rmn', block, picked.reshape(3, 1, NODES), precision=HIGHEST), None)
        total, unused = lax.scan(add_slot, jnp.zeros((3, 1, NODES), jnp.float32), (mats, source, weight))
        return field + jnp.einsum('rcn,cmn->rmn', inverse, total, precision=HIGHEST).reshape(3, NODES)
    earlier = start_vector
    current = start_vector
    for iteration in range(ITERS):
        earlier = current
        current = operator(current)
    rho = jnp.sqrt(jnp.sum(current * current) / (jnp.sum(earlier * earlier) + 1e-05))

    def slot_blocks(slot_data):
        block, anchor, scale = slot_data
        picked = (tentative[:, anchor] * scale[None, :]).reshape(3, 6, NODES)
        product = jnp.einsum('rcn,cmn->rmn', block, picked, precision=HIGHEST)
        scaled = jnp.einsum('rcn,cmn->rmn', inverse, product, precision=HIGHEST)
        return (-(OMEGA / rho) * scaled).reshape(18, NODES).astype(jnp.bfloat16)
    prolong_off = lax.map(slot_blocks, (mats, source, weight))
    prolong_self = ((1.0 - OMEGA / rho) * tentative).astype(jnp.bfloat16)
    return (prolong_off, prolong_self, rho)
```

```python
import functools

import jax
import jax.numpy as jnp
from jax import lax
from jax.experimental import pallas as pl
from jax.experimental.pallas import tpu as pltpu
from jax.sharding import PartitionSpec as P

ITERS = 8
OMEGA = 4.0 / 3.0
LANES = 128
MESH = pl.DeviceIdType.MESH


def lane_gather(table, lanes):
    return jnp.take_along_axis(table, lanes, axis=1, mode="promise_in_bounds")


def tile(number):
    return pl.ds(number * LANES, LANES)


def pick(tables, index, first):
    high = index >> 7
    low = index & (LANES - 1)
    out = jnp.zeros(index.shape, jnp.float32)
    for step, table in enumerate(tables):
        out = jnp.where(high == first + step, lane_gather(table, low), out)
    return out


def invert_rows(entries):
    cofactor = [
        entries[4] * entries[8] - entries[5] * entries[7],
        entries[5] * entries[6] - entries[3] * entries[8],
        entries[3] * entries[7] - entries[4] * entries[6],
        entries[2] * entries[7] - entries[1] * entries[8],
        entries[0] * entries[8] - entries[2] * entries[6],
        entries[1] * entries[6] - entries[0] * entries[7],
        entries[1] * entries[5] - entries[2] * entries[4],
        entries[2] * entries[3] - entries[0] * entries[5],
        entries[0] * entries[4] - entries[1] * entries[3],
    ]
    determinant = entries[0] * cofactor[0] + entries[1] * cofactor[1] + entries[2] * cofactor[2]
    return [
        cofactor[column * 3 + row] / determinant for row in range(3) for column in range(3)
    ]


def unit_places(slots, tiles):
    units = []
    for k in range(0, slots - 7, 8):
        for j in range(tiles):
            units.append([(0, k, 8, j)])
    rest = slots % 8
    if rest:
        share = 8 // rest
        for j in range(0, tiles, share):
            units.append(
                [
                    (rest * i, slots - rest, rest, j + i)
                    for i in range(min(share, tiles - j))
                ]
            )
    return units


def scale_kernel(raw_ref, tent_ref, rho_ref, off_ref, self_ref, out_rho_ref):
    slots, rows = off_ref.shape[1:]
    out_rho_ref[...] = rho_ref[...]
    inverse = OMEGA / rho_ref[...]
    factor = jnp.broadcast_to(-inverse, (8, LANES))
    places = unit_places(slots, rows // LANES)
    for j in range(rows // LANES):
        for entry in range(off_ref.shape[0]):
            parts = [
                (raw_ref[entry, u] * factor)[at : at + count]
                for u in range(len(places))
                for at, k, count, tile_number in places[u]
                if tile_number == j
            ]
            off_ref[entry, :, tile(j)] = jnp.concatenate(parts, axis=0).astype(off_ref.dtype)
    self_ref[...] = ((1.0 - inverse) * tent_ref[...]).astype(self_ref.dtype)


def kernel(
    n_slab, n_sub,
    near_hbm, agg_hbm, diag_hbm, off_hbm, cols_hbm, sends_hbm, start_hbm,
    raw_ref, tent_ref, rho_ref,
    near_ref, agg_ref, diag_ref, cols_ref, sends_ref, start_ref, off_v, cols_u, mats, dinv, text, hist, sidx,
    sendw, recvw, sendt, recvt, stat, stats,
    off_sem, sendw_sem, recvw_sem, sendt_sem, recvt_sem,
    ss_sem, rs_sem,
):
    slots, rows = cols_ref.shape
    half = sends_ref.shape[1]
    tiles = rows // LANES
    units = unit_places(slots, tiles)
    modes = near_ref.shape[0] // 3
    groups = rows // 8
    a = lax.axis_index("slab")
    b = lax.axis_index("sub")
    loads = [
        pltpu.make_async_copy(source, target, off_sem.at[number])
        for number, (source, target) in enumerate(
            (
                (start_hbm, start_ref),
                (sends_hbm, sends_ref),
                (agg_hbm, agg_ref),
                (near_hbm, near_ref),
                (diag_hbm, diag_ref),
                (cols_hbm, cols_ref),
                (off_hbm, off_v),
            )
        )
    ]
    for load in loads:
        load.start()

    recvw[...] = jnp.zeros_like(recvw)
    recvt[...] = jnp.zeros_like(recvt)
    barrier = pltpu.get_barrier_semaphore()

    def greet(step, unused):
        target = lax.rem(a * n_sub + b + step, n_slab * n_sub)
        pl.semaphore_signal(
            barrier, inc=1,
            device_id={"slab": lax.div(target, n_sub), "sub": lax.rem(target, n_sub)},
            device_id_type=MESH,
        )
        return unused

    lax.fori_loop(1, n_slab * n_sub, greet, 0)

    ways = (
        ("sub", b + 1, 0, b < n_sub - 1, b > 0),
        ("sub", b - 1, 0, b > 0, b < n_sub - 1),
        ("slab", a + 1, 1, a < n_slab - 1, a > 0),
        ("slab", a - 1, 1, a > 0, a < n_slab - 1),
    )

    def w_copy(t, way):
        axis, target, pair, unused, unused2 = ways[way]
        return pltpu.make_async_remote_copy(
            src_ref=sendw.at[t, pair], dst_ref=recvw.at[t, way],
            send_sem=sendw_sem.at[t, way], recv_sem=recvw_sem.at[t, way],
            device_id={axis: target}, device_id_type=MESH,
        )

    def t_copy(way):
        axis, target, pair, unused, unused2 = ways[way]
        return pltpu.make_async_remote_copy(
            src_ref=sendt.at[pair], dst_ref=recvt.at[way],
            send_sem=sendt_sem.at[way], recv_sem=recvt_sem.at[way],
            device_id={axis: target}, device_id_type=MESH,
        )

    def each_target(make, act):
        for way in range(4):
            pl.when(ways[way][3])(functools.partial(act, make, way))

    def each_source(make):
        for way in range(4):
            pl.when(ways[way][4])(functools.partial(lambda way: make(way).wait_recv(), way))

    hist[...] = jnp.zeros_like(hist)
    loads[0].wait()
    loads[1].wait()
    hist[0, 0:3, :] = start_ref[...]
    for pair in range(2):
        sidx[pair] = jnp.broadcast_to(
            jnp.concatenate(
                [sends_ref[2 * pair : 2 * pair + 1, :], sends_ref[2 * pair + 1 : 2 * pair + 2, :]],
                axis=1,
            ),
            (8, LANES),
        )

    def pack_w(t):
        tables = [hist[t, :, tile(j)] for j in range(tiles)]
        for pair in range(2):
            sendw[t, pair] = pick(tables, sidx[pair], 0)[0:4]

    pack_w(0)

    loads[2].wait()
    loads[3].wait()
    agg = agg_ref[...]
    member = (
        jnp.broadcast_to(agg, (groups, rows)) == lax.broadcasted_iota(jnp.int32, (groups, rows), 0)
    ).astype(jnp.float32)
    counts = jnp.sum(member, axis=1, keepdims=True)
    sizes = jnp.sum(member * counts, axis=0, keepdims=True)
    tent = near_ref[...] * lax.rsqrt(sizes)
    tent_ref[...] = tent
    text[...] = jnp.zeros_like(text)
    for c in range(3):
        text[8 * c : 8 * c + modes, 0:rows] = tent_ref[modes * c : modes * (c + 1), :]
    for pair in range(2):
        for c in range(3):
            sendt[pair, 8 * c : 8 * c + 8, :] = pick(
                [text[8 * c : 8 * c + 8, tile(j)] for j in range(tiles)], sidx[pair], 0
            )

    loads[4].wait()
    loads[5].wait()
    for u, places in enumerate(units):
        if len(places) * places[0][2] < 8:
            cols_u[u] = jnp.zeros((8, LANES), jnp.int32)
        for at, k, count, j in places:
            cols_u[u, at : at + count, :] = cols_ref[k : k + count, tile(j)]

    inverse = invert_rows([diag_ref[p : p + 1, :] for p in range(9)])
    for p in range(9):
        dinv[p : p + 1, :] = inverse[p]
    pl.semaphore_wait(barrier, n_slab * n_sub - 1)
    each_target(functools.partial(w_copy, 0), lambda make, way: make(way).start())
    each_target(t_copy, lambda make, way: make(way).start())
    loads[6].wait()
    for u, places in enumerate(units):
        if len(places) * places[0][2] < 8:
            mats[u] = jnp.zeros(mats.shape[1:], jnp.float32)
        for at, k, count, j in places:
            block = [off_v[p, k : k + count, tile(j)] for p in range(9)]
            for r in range(3):
                scale = [
                    jnp.broadcast_to(dinv[3 * r + q : 3 * r + q + 1, tile(j)], (count, LANES))
                    for q in range(3)
                ]
                for c in range(3):
                    mats[u, 3 * r + c, at : at + count, :] = (
                        scale[0] * block[c] + scale[1] * block[3 + c] + scale[2] * block[6 + c]
                    )

    left = lax.broadcasted_iota(jnp.int32, (8, LANES), 1) < half
    per = -(-len(units) // (ITERS - 1))

    def unit_products(u, unused):
        index = cols_u[u]
        for m in range(modes):
            picked = [
                pick(
                    [
                        jnp.broadcast_to(text[8 * c + m : 8 * c + m + 1, tile(i)], (8, LANES))
                        for i in range(tiles + 2)
                    ],
                    index,
                    0,
                )
                for c in range(3)
            ]
            for r in range(3):
                raw_ref[modes * r + m, u] = (
                    mats[u, 3 * r] * picked[0]
                    + mats[u, 3 * r + 1] * picked[1]
                    + mats[u, 3 * r + 2] * picked[2]
                )
        return unused

    def contribute(tables, first, u):
        index = cols_u[u]
        picked = [pick(tables[c], index, first) for c in range(3)]
        return [sum(mats[u, 3 * r + c] * picked[c] for c in range(3)) for r in range(3)]

    def by_tile(terms):
        whole = [[None] * tiles for r in range(3)]
        for r in range(3):
            for u, places in enumerate(units):
                if len(places) == 1 and places[0][2] == 8:
                    j = places[0][3]
                    old = whole[r][j]
                    whole[r][j] = terms[u][r] if old is None else old + terms[u][r]
            for j in range(tiles):
                old = whole[r][j]
                whole[r][j] = 0.0 if old is None else jnp.sum(old, axis=0, keepdims=True)
            for u, places in enumerate(units):
                if not (len(places) == 1 and places[0][2] == 8):
                    for at, k, count, j in places:
                        whole[r][j] = whole[r][j] + jnp.sum(
                            terms[u][r][at : at + count], axis=0, keepdims=True
                        )
        return whole

    def iterate(t, unused):
        local = [
            [jnp.broadcast_to(hist[t, c : c + 1, tile(i)], (8, LANES)) for i in range(tiles)]
            for c in range(3)
        ]
        inner = by_tile([contribute(local, 0, u) for u in range(len(units))])
        for r in range(3):
            for j in range(tiles):
                hist[t + 1, r : r + 1, tile(j)] = hist[t, r : r + 1, tile(j)] + inner[r][j]

        @pl.when(t == 1)
        def _():
            each_source(t_copy)
            for pair in range(2):
                for c in range(3):
                    text[8 * c : 8 * c + 8, tile(tiles + pair)] = jnp.where(
                        left,
                        recvt[2 * pair, 8 * c : 8 * c + 8, :],
                        recvt[2 * pair + 1, 8 * c : 8 * c + 8, :],
                    )

        lax.fori_loop(
            jnp.clip((t - 1) * per, 0, len(units)), jnp.clip(t * per, 0, len(units)), unit_products, 0
        )
        each_source(functools.partial(w_copy, t))
        merged = [jnp.where(left[0:4], recvw[t, 2 * pair], recvw[t, 2 * pair + 1]) for pair in range(2)]
        ghost = [
            [jnp.broadcast_to(merged[pair][c : c + 1], (8, LANES)) for pair in range(2)]
            for c in range(3)
        ]
        outer = by_tile([contribute(ghost, tiles, u) for u in range(len(units))])
        for r in range(3):
            for j in range(tiles):
                hist[t + 1, r : r + 1, tile(j)] = hist[t + 1, r : r + 1, tile(j)] + outer[r][j]

        @pl.when(t < ITERS - 1)
        def _():
            pack_w(t + 1)
            each_target(functools.partial(w_copy, t + 1), lambda make, way: make(way).start())

        return unused

    lax.fori_loop(0, ITERS, iterate, 0)


    def squares(t):
        return jnp.sum(
            sum(hist[t, :, tile(j)] * hist[t, :, tile(j)] for j in range(tiles)), keepdims=True
        )

    lane = lax.broadcasted_iota(jnp.int32, (1, LANES), 1)
    latest = jnp.broadcast_to(squares(ITERS), (1, LANES))
    previous = jnp.broadcast_to(squares(ITERS - 1), (1, LANES))
    own = jnp.where(lane == 0, latest, jnp.where(lane == 1, previous, 0.0))
    me = a * n_sub + b
    devices = n_slab * n_sub
    stat[0] = own

    def stat_copy(step, source):
        target = lax.rem(me + step, devices)
        landing = lax.rem(me + devices - step, devices) if source else me
        return pltpu.make_async_remote_copy(
            src_ref=stat.at[0], dst_ref=stats.at[landing],
            send_sem=ss_sem.at[step], recv_sem=rs_sem.at[landing],
            device_id={"slab": lax.div(target, n_sub), "sub": lax.rem(target, n_sub)},
            device_id_type=MESH,
        )

    def begin(step, unused):
        stat_copy(step, False).start()
        return unused

    def arrive(step, unused):
        stat_copy(step, True).wait_recv()
        return unused

    def sent(step, unused):
        stat_copy(step, False).wait_send()
        return unused

    lax.fori_loop(1, devices, begin, 0)
    stats[me] = own
    lax.fori_loop(1, devices, arrive, 0)
    whole = jnp.sum(stats[...], axis=0)
    latest = whole[:, 0:1]
    previous = whole[:, 1:2]
    rho_ref[...] = jnp.sqrt(latest / (previous + 1e-05))

    lax.fori_loop(1, devices, sent, 0)
    each_target(t_copy, lambda make, way: make(way).wait_send())

    def drain(t, unused):
        each_target(functools.partial(w_copy, t), lambda make, way: make(way).wait_send())
        return unused

    lax.fori_loop(0, ITERS, drain, 0)


def body(n_slab, n_sub, near_null, aggregates, diag_block, off_blocks, columns, sends, start_vector):
    slots, nine, rows = off_blocks.shape
    wide = rows + 2 * LANES
    count = len(unit_places(slots, rows // LANES))
    f32 = jnp.float32
    vmem = pl.BlockSpec(memory_space=pltpu.VMEM)
    dma = pltpu.SemaphoreType.DMA
    raw, tentative, rho = pl.pallas_call(
        functools.partial(kernel, n_slab, n_sub),
        out_shape=(
            pltpu.VMEM((near_null.shape[0], count, 8, LANES), f32),
            pltpu.VMEM(near_null.shape, f32),
            jax.ShapeDtypeStruct((1, 1), f32),
        ),
        in_specs=[pl.BlockSpec(memory_space=pltpu.HBM)] * 7,
        out_specs=(vmem, vmem, vmem),
        scratch_shapes=[
            pltpu.VMEM(near_null.shape, f32),
            pltpu.VMEM((1, rows), jnp.int32),
            pltpu.VMEM(diag_block.shape, f32),
            pltpu.VMEM(columns.shape, jnp.int32),
            pltpu.VMEM(sends.shape, jnp.int32),
            pltpu.VMEM(start_vector.shape, f32),
            pltpu.VMEM((nine, slots, rows), f32),
            pltpu.VMEM((count, 8, LANES), jnp.int32),
            pltpu.VMEM((count, nine, 8, LANES), f32),
            pltpu.VMEM((16, rows), f32),
            pltpu.VMEM((24, wide), f32),
            pltpu.VMEM((ITERS + 1, 8, rows), f32),
            pltpu.VMEM((2, 8, LANES), jnp.int32),
            pltpu.VMEM((ITERS, 2, 4, LANES), f32),
            pltpu.VMEM((ITERS, 4, 4, LANES), f32),
            pltpu.VMEM((2, 24, LANES), f32),
            pltpu.VMEM((4, 24, LANES), f32),
            pltpu.VMEM((1, 1, LANES), f32),
            pltpu.VMEM((n_slab * n_sub, 1, LANES), f32),
            dma((7,)),
            dma((ITERS, 4)),
            dma((ITERS, 4)),
            dma((4,)),
            dma((4,)),
            dma((n_slab * n_sub,)),
            dma((n_slab * n_sub,)),
        ],
        compiler_params=pltpu.CompilerParams(collective_id=0, has_side_effects=True, vmem_limit_bytes=16777216),
        name="smooth",
    )(
        *[
            pltpu.with_memory_space_constraint(x, pltpu.HBM)
            for x in (
                near_null, aggregates.reshape(1, rows), diag_block, off_blocks.transpose(1, 0, 2),
                columns, sends, start_vector,
            )
        ]
    )
    prolong_off, prolong_self, rho = pl.pallas_call(
        scale_kernel,
        out_shape=(
            jax.ShapeDtypeStruct((near_null.shape[0], slots, rows), jnp.bfloat16),
            jax.ShapeDtypeStruct(near_null.shape, jnp.bfloat16),
            jax.ShapeDtypeStruct((1, 1), f32),
        ),
        in_specs=[vmem, vmem, vmem],
        out_specs=(vmem, vmem, vmem),
        compiler_params=pltpu.CompilerParams(vmem_limit_bytes=16777216),
        name="scale",
    )(raw, tentative, rho)
    return (prolong_off.transpose(1, 0, 2), prolong_self, rho.reshape(()))


def solution(mesh):
    placed = (
        P(None, ("slab", "sub")),
        P(("slab", "sub")),
        P(None, ("slab", "sub")),
        P(None, None, ("slab", "sub")),
        P(None, ("slab", "sub")),
        P(None, ("slab", "sub")),
        P(None, ("slab", "sub")),
    )
    return jax.shard_map(
        functools.partial(body, mesh.shape["slab"], mesh.shape["sub"]),
        mesh=mesh,
        in_specs=placed,
        out_specs=(P(None, None, ("slab", "sub")), P(None, ("slab", "sub")), P()),
        check_vma=False,
    )
```

```python
import functools

import jax
import jax.numpy as jnp
from jax import lax
from jax.experimental import pallas as pl
from jax.experimental.pallas import tpu as pltpu
from jax.sharding import PartitionSpec as P

ITERS = 8
OMEGA = 4.0 / 3.0
LANES = 128
MESH = pl.DeviceIdType.MESH
CIRCLE = [
    (x, y) for x in range(-2, 3) for y in range(-2, 3) if 1 <= abs(x) + abs(y) <= 2
]


def lane_gather(table, lanes):
    return jnp.take_along_axis(table, lanes, axis=1, mode="promise_in_bounds")


def tile(number):
    return pl.ds(number * LANES, LANES)


def pick(tables, index, first):
    high = index >> 7
    low = index & (LANES - 1)
    out = jnp.zeros(index.shape, jnp.float32)
    for step, table in enumerate(tables):
        out = jnp.where(high == first + step, lane_gather(table, low), out)
    return out


def invert_rows(entries):
    cofactor = [
        entries[4] * entries[8] - entries[5] * entries[7],
        entries[5] * entries[6] - entries[3] * entries[8],
        entries[3] * entries[7] - entries[4] * entries[6],
        entries[2] * entries[7] - entries[1] * entries[8],
        entries[0] * entries[8] - entries[2] * entries[6],
        entries[1] * entries[6] - entries[0] * entries[7],
        entries[1] * entries[5] - entries[2] * entries[4],
        entries[2] * entries[3] - entries[0] * entries[5],
        entries[0] * entries[4] - entries[1] * entries[3],
    ]
    determinant = entries[0] * cofactor[0] + entries[1] * cofactor[1] + entries[2] * cofactor[2]
    return [
        cofactor[column * 3 + row] / determinant for row in range(3) for column in range(3)
    ]


def unit_places(slots, tiles):
    units = []
    for k in range(0, slots - 7, 8):
        for j in range(tiles):
            units.append([(0, k, 8, j)])
    rest = slots % 8
    if rest:
        share = 8 // rest
        for j in range(0, tiles, share):
            units.append(
                [
                    (rest * i, slots - rest, rest, j + i)
                    for i in range(min(share, tiles - j))
                ]
            )
    return units


def scale_kernel(raw_ref, tent_ref, rho_ref, off_ref, self_ref, out_rho_ref):
    slots, rows = off_ref.shape[1:]
    out_rho_ref[...] = rho_ref[...]
    inverse = OMEGA / rho_ref[...]
    factor = jnp.broadcast_to(-inverse, (8, LANES))
    places = unit_places(slots, rows // LANES)
    for j in range(rows // LANES):
        for entry in range(off_ref.shape[0]):
            parts = [
                (raw_ref[entry, u] * factor)[at : at + count]
                for u in range(len(places))
                for at, k, count, tile_number in places[u]
                if tile_number == j
            ]
            off_ref[entry, :, tile(j)] = jnp.concatenate(parts, axis=0).astype(off_ref.dtype)
    self_ref[...] = ((1.0 - inverse) * tent_ref[...]).astype(self_ref.dtype)


def kernel(
    n_slab, n_sub,
    near_hbm, agg_hbm, diag_hbm, off_hbm, cols_hbm, sends_hbm, start_hbm,
    raw_ref, tent_ref, rho_ref,
    near_ref, agg_ref, diag_ref, cols_ref, sends_ref, start_ref, off_v, cols_u, mats, dinv, text, hist, sidx,
    sendw, recvw, sendt, recvt, stat, stats,
    off_sem, sendw_sem, recvw_sem, sendt_sem, recvt_sem,
    ss_sem, rs_sem,
):
    slots, rows = cols_ref.shape
    half = sends_ref.shape[1]
    tiles = rows // LANES
    units = unit_places(slots, tiles)
    modes = near_ref.shape[0] // 3
    groups = rows // 8
    a = lax.axis_index("slab")
    b = lax.axis_index("sub")
    loads = [
        pltpu.make_async_copy(source, target, off_sem.at[number])
        for number, (source, target) in enumerate(
            (
                (start_hbm, start_ref),
                (sends_hbm, sends_ref),
                (agg_hbm, agg_ref),
                (near_hbm, near_ref),
                (diag_hbm, diag_ref),
                (cols_hbm, cols_ref),
                (off_hbm, off_v),
            )
        )
    ]
    for load in loads:
        load.start()

    recvw[...] = jnp.zeros_like(recvw)
    recvt[...] = jnp.zeros_like(recvt)
    barrier = pltpu.get_barrier_semaphore()

    def present(x, y):
        return (a + x >= 0) & (a + x < n_slab) & (b + y >= 0) & (b + y < n_sub)

    def greet(x, y):
        pl.semaphore_signal(
            barrier, inc=1, device_id={"slab": a + x, "sub": b + y}, device_id_type=MESH
        )

    def greet_any(step, unused):
        target = lax.rem(a * n_sub + b + step, n_slab * n_sub)
        greet(lax.div(target, n_sub) - a, lax.rem(target, n_sub) - b)
        return unused

    near = n_slab - 1 + n_sub - 1 <= ITERS + 2
    if near:
        for x, y in CIRCLE:
            pl.when(present(x, y))(functools.partial(greet, x, y))
        greeters = sum(present(x, y).astype(jnp.int32) for x, y in CIRCLE)
    else:
        lax.fori_loop(1, n_slab * n_sub, greet_any, 0)
        greeters = n_slab * n_sub - 1

    ways = (
        ("sub", b + 1, 0, b < n_sub - 1, b > 0),
        ("sub", b - 1, 0, b > 0, b < n_sub - 1),
        ("slab", a + 1, 1, a < n_slab - 1, a > 0),
        ("slab", a - 1, 1, a > 0, a < n_slab - 1),
    )

    def w_copy(t, way):
        axis, target, pair, unused, unused2 = ways[way]
        return pltpu.make_async_remote_copy(
            src_ref=sendw.at[t, pair], dst_ref=recvw.at[t, way],
            send_sem=sendw_sem.at[t, way], recv_sem=recvw_sem.at[t, way],
            device_id={axis: target}, device_id_type=MESH,
        )

    def t_copy(way):
        axis, target, pair, unused, unused2 = ways[way]
        return pltpu.make_async_remote_copy(
            src_ref=sendt.at[pair], dst_ref=recvt.at[way],
            send_sem=sendt_sem.at[way], recv_sem=recvt_sem.at[way],
            device_id={axis: target}, device_id_type=MESH,
        )

    def each_target(make, act):
        for way in range(4):
            pl.when(ways[way][3])(functools.partial(act, make, way))

    def each_source(make):
        for way in range(4):
            pl.when(ways[way][4])(functools.partial(lambda way: make(way).wait_recv(), way))

    hist[...] = jnp.zeros_like(hist)
    loads[0].wait()
    loads[1].wait()
    hist[0, 0:3, :] = start_ref[...]
    for pair in range(2):
        sidx[pair] = jnp.broadcast_to(
            jnp.concatenate(
                [sends_ref[2 * pair : 2 * pair + 1, :], sends_ref[2 * pair + 1 : 2 * pair + 2, :]],
                axis=1,
            ),
            (8, LANES),
        )

    def pack_w(t):
        tables = [hist[t, :, tile(j)] for j in range(tiles)]
        for pair in range(2):
            sendw[t, pair] = pick(tables, sidx[pair], 0)[0:4]

    pack_w(0)

    loads[2].wait()
    loads[3].wait()
    agg = agg_ref[...]
    member = (
        jnp.broadcast_to(agg, (groups, rows)) == lax.broadcasted_iota(jnp.int32, (groups, rows), 0)
    ).astype(jnp.float32)
    counts = jnp.sum(member, axis=1, keepdims=True)
    sizes = jnp.sum(member * counts, axis=0, keepdims=True)
    tent = near_ref[...] * lax.rsqrt(sizes)
    tent_ref[...] = tent
    text[...] = jnp.zeros_like(text)
    for c in range(3):
        text[8 * c : 8 * c + modes, 0:rows] = tent_ref[modes * c : modes * (c + 1), :]
    for pair in range(2):
        for c in range(3):
            sendt[pair, 8 * c : 8 * c + 8, :] = pick(
                [text[8 * c : 8 * c + 8, tile(j)] for j in range(tiles)], sidx[pair], 0
            )

    loads[4].wait()
    loads[5].wait()
    for u, places in enumerate(units):
        if len(places) * places[0][2] < 8:
            cols_u[u] = jnp.zeros((8, LANES), jnp.int32)
        for at, k, count, j in places:
            cols_u[u, at : at + count, :] = cols_ref[k : k + count, tile(j)]

    inverse = invert_rows([diag_ref[p : p + 1, :] for p in range(9)])
    for p in range(9):
        dinv[p : p + 1, :] = inverse[p]
    pl.semaphore_wait(barrier, greeters)
    each_target(functools.partial(w_copy, 0), lambda make, way: make(way).start())
    each_target(t_copy, lambda make, way: make(way).start())
    loads[6].wait()
    for u, places in enumerate(units):
        if len(places) * places[0][2] < 8:
            mats[u] = jnp.zeros(mats.shape[1:], jnp.float32)
        for at, k, count, j in places:
            block = [off_v[p, k : k + count, tile(j)] for p in range(9)]
            for r in range(3):
                scale = [
                    jnp.broadcast_to(dinv[3 * r + q : 3 * r + q + 1, tile(j)], (count, LANES))
                    for q in range(3)
                ]
                for c in range(3):
                    mats[u, 3 * r + c, at : at + count, :] = (
                        scale[0] * block[c] + scale[1] * block[3 + c] + scale[2] * block[6 + c]
                    )

    left = lax.broadcasted_iota(jnp.int32, (8, LANES), 1) < half
    per = -(-len(units) // (ITERS - 1))

    def unit_products(u, unused):
        index = cols_u[u]
        for m in range(modes):
            picked = [
                pick(
                    [
                        jnp.broadcast_to(text[8 * c + m : 8 * c + m + 1, tile(i)], (8, LANES))
                        for i in range(tiles + 2)
                    ],
                    index,
                    0,
                )
                for c in range(3)
            ]
            for r in range(3):
                raw_ref[modes * r + m, u] = (
                    mats[u, 3 * r] * picked[0]
                    + mats[u, 3 * r + 1] * picked[1]
                    + mats[u, 3 * r + 2] * picked[2]
                )
        return unused

    def contribute(tables, first, u):
        index = cols_u[u]
        picked = [pick(tables[c], index, first) for c in range(3)]
        return [sum(mats[u, 3 * r + c] * picked[c] for c in range(3)) for r in range(3)]

    def by_tile(terms):
        whole = [[None] * tiles for r in range(3)]
        for r in range(3):
            for u, places in enumerate(units):
                if len(places) == 1 and places[0][2] == 8:
                    j = places[0][3]
                    old = whole[r][j]
                    whole[r][j] = terms[u][r] if old is None else old + terms[u][r]
            for j in range(tiles):
                old = whole[r][j]
                whole[r][j] = 0.0 if old is None else jnp.sum(old, axis=0, keepdims=True)
            for u, places in enumerate(units):
                if not (len(places) == 1 and places[0][2] == 8):
                    for at, k, count, j in places:
                        whole[r][j] = whole[r][j] + jnp.sum(
                            terms[u][r][at : at + count], axis=0, keepdims=True
                        )
        return whole

    def iterate(t, unused):
        local = [
            [jnp.broadcast_to(hist[t, c : c + 1, tile(i)], (8, LANES)) for i in range(tiles)]
            for c in range(3)
        ]
        inner = by_tile([contribute(local, 0, u) for u in range(len(units))])
        for r in range(3):
            for j in range(tiles):
                hist[t + 1, r : r + 1, tile(j)] = hist[t, r : r + 1, tile(j)] + inner[r][j]

        @pl.when(t == 1)
        def _():
            each_source(t_copy)
            for pair in range(2):
                for c in range(3):
                    text[8 * c : 8 * c + 8, tile(tiles + pair)] = jnp.where(
                        left,
                        recvt[2 * pair, 8 * c : 8 * c + 8, :],
                        recvt[2 * pair + 1, 8 * c : 8 * c + 8, :],
                    )

        lax.fori_loop(
            jnp.clip((t - 1) * per, 0, len(units)), jnp.clip(t * per, 0, len(units)), unit_products, 0
        )
        each_source(functools.partial(w_copy, t))
        merged = [jnp.where(left[0:4], recvw[t, 2 * pair], recvw[t, 2 * pair + 1]) for pair in range(2)]
        ghost = [
            [jnp.broadcast_to(merged[pair][c : c + 1], (8, LANES)) for pair in range(2)]
            for c in range(3)
        ]
        outer = by_tile([contribute(ghost, tiles, u) for u in range(len(units))])
        for r in range(3):
            for j in range(tiles):
                hist[t + 1, r : r + 1, tile(j)] = hist[t + 1, r : r + 1, tile(j)] + outer[r][j]

        @pl.when(t < ITERS - 1)
        def _():
            pack_w(t + 1)
            each_target(functools.partial(w_copy, t + 1), lambda make, way: make(way).start())

        return unused

    lax.fori_loop(0, ITERS, iterate, 0)


    def squares(t):
        return jnp.sum(
            sum(hist[t, :, tile(j)] * hist[t, :, tile(j)] for j in range(tiles)), keepdims=True
        )

    lane = lax.broadcasted_iota(jnp.int32, (1, LANES), 1)
    latest = jnp.broadcast_to(squares(ITERS), (1, LANES))
    previous = jnp.broadcast_to(squares(ITERS - 1), (1, LANES))
    own = jnp.where(lane == 0, latest, jnp.where(lane == 1, previous, 0.0))
    me = a * n_sub + b
    devices = n_slab * n_sub
    stat[0] = own

    def stat_copy(step, source):
        target = lax.rem(me + step, devices)
        landing = lax.rem(me + devices - step, devices) if source else me
        return pltpu.make_async_remote_copy(
            src_ref=stat.at[0], dst_ref=stats.at[landing],
            send_sem=ss_sem.at[step], recv_sem=rs_sem.at[landing],
            device_id={"slab": lax.div(target, n_sub), "sub": lax.rem(target, n_sub)},
            device_id_type=MESH,
        )

    def begin(step, unused):
        stat_copy(step, False).start()
        return unused

    def arrive(step, unused):
        stat_copy(step, True).wait_recv()
        return unused

    def sent(step, unused):
        stat_copy(step, False).wait_send()
        return unused

    lax.fori_loop(1, devices, begin, 0)
    stats[me] = own
    lax.fori_loop(1, devices, arrive, 0)
    whole = jnp.sum(stats[...], axis=0)
    latest = whole[:, 0:1]
    previous = whole[:, 1:2]
    rho_ref[...] = jnp.sqrt(latest / (previous + 1e-05))

    lax.fori_loop(1, devices, sent, 0)
    each_target(t_copy, lambda make, way: make(way).wait_send())

    def drain(t, unused):
        each_target(functools.partial(w_copy, t), lambda make, way: make(way).wait_send())
        return unused

    lax.fori_loop(0, ITERS, drain, 0)


def body(n_slab, n_sub, near_null, aggregates, diag_block, off_blocks, columns, sends, start_vector):
    slots, nine, rows = off_blocks.shape
    wide = rows + 2 * LANES
    count = len(unit_places(slots, rows // LANES))
    f32 = jnp.float32
    vmem = pl.BlockSpec(memory_space=pltpu.VMEM)
    dma = pltpu.SemaphoreType.DMA
    raw, tentative, rho = pl.pallas_call(
        functools.partial(kernel, n_slab, n_sub),
        out_shape=(
            pltpu.VMEM((near_null.shape[0], count, 8, LANES), f32),
            pltpu.VMEM(near_null.shape, f32),
            jax.ShapeDtypeStruct((1, 1), f32),
        ),
        in_specs=[pl.BlockSpec(memory_space=pltpu.HBM)] * 7,
        out_specs=(vmem, vmem, vmem),
        scratch_shapes=[
            pltpu.VMEM(near_null.shape, f32),
            pltpu.VMEM((1, rows), jnp.int32),
            pltpu.VMEM(diag_block.shape, f32),
            pltpu.VMEM(columns.shape, jnp.int32),
            pltpu.VMEM(sends.shape, jnp.int32),
            pltpu.VMEM(start_vector.shape, f32),
            pltpu.VMEM((nine, slots, rows), f32),
            pltpu.VMEM((count, 8, LANES), jnp.int32),
            pltpu.VMEM((count, nine, 8, LANES), f32),
            pltpu.VMEM((16, rows), f32),
            pltpu.VMEM((24, wide), f32),
            pltpu.VMEM((ITERS + 1, 8, rows), f32),
            pltpu.VMEM((2, 8, LANES), jnp.int32),
            pltpu.VMEM((ITERS, 2, 4, LANES), f32),
            pltpu.VMEM((ITERS, 4, 4, LANES), f32),
            pltpu.VMEM((2, 24, LANES), f32),
            pltpu.VMEM((4, 24, LANES), f32),
            pltpu.VMEM((1, 1, LANES), f32),
            pltpu.VMEM((n_slab * n_sub, 1, LANES), f32),
            dma((7,)),
            dma((ITERS, 4)),
            dma((ITERS, 4)),
            dma((4,)),
            dma((4,)),
            dma((n_slab * n_sub,)),
            dma((n_slab * n_sub,)),
        ],
        compiler_params=pltpu.CompilerParams(collective_id=0, has_side_effects=True, vmem_limit_bytes=16777216),
        name="smooth",
    )(
        *[
            pltpu.with_memory_space_constraint(x, pltpu.HBM)
            for x in (
                near_null, aggregates.reshape(1, rows), diag_block, off_blocks.transpose(1, 0, 2),
                columns, sends, start_vector,
            )
        ]
    )
    prolong_off, prolong_self, rho = pl.pallas_call(
        scale_kernel,
        out_shape=(
            jax.ShapeDtypeStruct((near_null.shape[0], slots, rows), jnp.bfloat16),
            jax.ShapeDtypeStruct(near_null.shape, jnp.bfloat16),
            jax.ShapeDtypeStruct((1, 1), f32),
        ),
        in_specs=[vmem, vmem, vmem],
        out_specs=(vmem, vmem, vmem),
        compiler_params=pltpu.CompilerParams(vmem_limit_bytes=16777216),
        name="scale",
    )(raw, tentative, rho)
    return (prolong_off.transpose(1, 0, 2), prolong_self, rho.reshape(()))


def solution(mesh):
    placed = (
        P(None, ("slab", "sub")),
        P(("slab", "sub")),
        P(None, ("slab", "sub")),
        P(None, None, ("slab", "sub")),
        P(None, ("slab", "sub")),
        P(None, ("slab", "sub")),
        P(None, ("slab", "sub")),
    )
    return jax.shard_map(
        functools.partial(body, mesh.shape["slab"], mesh.shape["sub"]),
        mesh=mesh,
        in_specs=placed,
        out_specs=(P(None, None, ("slab", "sub")), P(None, ("slab", "sub")), P()),
        check_vma=False,
    )
```

```python
import functools

import jax
import jax.numpy as jnp
from jax import lax
from jax.experimental import pallas as pl
from jax.experimental.pallas import tpu as pltpu
from jax.sharding import PartitionSpec as P

ITERS = 8
OMEGA = 4.0 / 3.0
LANES = 128
MESH = pl.DeviceIdType.MESH
DEPTH = 2
BLOCKS = ITERS // DEPTH
WAYS = [(0, 1), (0, -1), (1, 0), (-1, 0)]
FAR = [(-1, -1), (-1, 1), (1, -1), (1, 1), (-2, 0), (2, 0), (0, -2), (0, 2)]
CIRCLE = WAYS + FAR
ORDER = list(range(len(WAYS), len(CIRCLE))) + list(range(len(WAYS)))


def lane_gather(table, lanes):
    return jnp.take_along_axis(table, lanes, axis=1, mode="promise_in_bounds")


def tile(number):
    return pl.ds(number * LANES, LANES)


def pick(tables, index, first):
    high = index >> 7
    low = index & (LANES - 1)
    out = jnp.zeros(index.shape, jnp.float32)
    for step, table in enumerate(tables):
        out = jnp.where(high == first + step, lane_gather(table, low), out)
    return out


def invert_rows(entries):
    cofactor = [
        entries[4] * entries[8] - entries[5] * entries[7],
        entries[5] * entries[6] - entries[3] * entries[8],
        entries[3] * entries[7] - entries[4] * entries[6],
        entries[2] * entries[7] - entries[1] * entries[8],
        entries[0] * entries[8] - entries[2] * entries[6],
        entries[1] * entries[6] - entries[0] * entries[7],
        entries[1] * entries[5] - entries[2] * entries[4],
        entries[2] * entries[3] - entries[0] * entries[5],
        entries[0] * entries[4] - entries[1] * entries[3],
    ]
    determinant = entries[0] * cofactor[0] + entries[1] * cofactor[1] + entries[2] * cofactor[2]
    return [
        cofactor[column * 3 + row] / determinant for row in range(3) for column in range(3)
    ]


def unit_places(slots, tiles):
    units = []
    for k in range(0, slots - 7, 8):
        for j in range(tiles):
            units.append([(0, k, 8, j)])
    rest = slots % 8
    if rest:
        share = 8 // rest
        for j in range(0, tiles, share):
            units.append(
                [
                    (rest * i, slots - rest, rest, j + i)
                    for i in range(min(share, tiles - j))
                ]
            )
    return units


def scale_kernel(raw_ref, tent_ref, rho_ref, off_ref, self_ref, out_rho_ref):
    slots, rows = off_ref.shape[1:]
    out_rho_ref[...] = rho_ref[...]
    inverse = OMEGA / rho_ref[...]
    factor = jnp.broadcast_to(-inverse, (8, LANES))
    places = unit_places(slots, rows // LANES)
    for j in range(rows // LANES):
        for entry in range(off_ref.shape[0]):
            parts = [
                (raw_ref[entry, u] * factor)[at : at + count]
                for u in range(len(places))
                for at, k, count, tile_number in places[u]
                if tile_number == j
            ]
            off_ref[entry, :, tile(j)] = jnp.concatenate(parts, axis=0).astype(off_ref.dtype)
    self_ref[...] = ((1.0 - inverse) * tent_ref[...]).astype(self_ref.dtype)


def kernel(
    n_slab, n_sub,
    near_hbm, agg_hbm, diag_hbm, off_hbm, cols_hbm, sends_hbm, start_hbm,
    raw_ref, tent_ref, rho_ref,
    near_ref, agg_ref, diag_ref, cols_ref, sends_ref, start_ref, off_v, cols_u, mats, rest_m, dinv, text, hist, sidx,
    sendw, recvw, recvp, sendg, recvg, gcol, sendt, recvt, stat, stats,
    off_sem, sendw_sem, recvw_sem, sendg_sem, recvg_sem, sendt_sem, recvt_sem,
    ss_sem, rs_sem,
):
    slots, rows = cols_ref.shape
    half = sends_ref.shape[1]
    tiles = rows // LANES
    units = unit_places(slots, tiles)
    groups = -(-slots // 8)
    gunits, planes = sendg.shape[1:3]
    modes = near_ref.shape[0] // 3
    sizes_of = rows // 8
    a = lax.axis_index("slab")
    b = lax.axis_index("sub")
    loads = [
        pltpu.make_async_copy(source, target, off_sem.at[number])
        for number, (source, target) in enumerate(
            (
                (start_hbm, start_ref),
                (sends_hbm, sends_ref),
                (agg_hbm, agg_ref),
                (near_hbm, near_ref),
                (diag_hbm, diag_ref),
                (cols_hbm, cols_ref),
                (off_hbm, off_v),
            )
        )
    ]
    for load in loads:
        load.start()

    barrier = pltpu.get_barrier_semaphore()

    def present(x, y):
        return (a + x >= 0) & (a + x < n_slab) & (b + y >= 0) & (b + y < n_sub)

    def greet(x, y):
        pl.semaphore_signal(
            barrier, inc=1, device_id={"slab": a + x, "sub": b + y}, device_id_type=MESH
        )

    def greet_any(step, unused):
        target = lax.rem(a * n_sub + b + step, n_slab * n_sub)
        greet(lax.div(target, n_sub) - a, lax.rem(target, n_sub) - b)
        return unused

    near = n_slab - 1 + n_sub - 1 <= ITERS + 2
    if near:
        for x, y in CIRCLE:
            pl.when(present(x, y))(functools.partial(greet, x, y))
        greeters = sum(present(x, y).astype(jnp.int32) for x, y in CIRCLE)
    else:
        lax.fori_loop(1, n_slab * n_sub, greet_any, 0)
        greeters = n_slab * n_sub - 1

    def clear(place):
        if place < len(WAYS):
            for ref in (recvw.at[:, place], recvg.at[place], recvt.at[place]):
                ref[...] = jnp.zeros(ref.shape, jnp.float32)
        else:
            ref = recvp.at[:, place - len(WAYS)]
            ref[...] = jnp.zeros(ref.shape, jnp.float32)

    for place, (x, y) in enumerate(CIRCLE):
        pl.when(jnp.logical_not(present(-x, -y)))(functools.partial(clear, place))

    def remote(source, target, sent, came, place):
        x, y = CIRCLE[place]
        return pltpu.make_async_remote_copy(
            src_ref=source, dst_ref=target, send_sem=sent, recv_sem=came,
            device_id={"slab": a + x, "sub": b + y}, device_id_type=MESH,
        )

    def w_copy(turn, place):
        if place < len(WAYS):
            source, target = sendw.at[turn], recvw.at[turn, place]
        else:
            source, target = sendw.at[turn, 0], recvp.at[turn, place - len(WAYS)]
        return remote(source, target, sendw_sem.at[turn, place], recvw_sem.at[turn, place], place)

    def g_copy(way):
        return remote(sendg.at[way], recvg.at[way], sendg_sem.at[way], recvg_sem.at[way], way)

    def t_copy(way):
        return remote(sendt.at[way // 2], recvt.at[way], sendt_sem.at[way], recvt_sem.at[way], way)

    def each_target(make, places, act):
        for place in places:
            x, y = CIRCLE[place]
            pl.when(present(x, y))(functools.partial(lambda place: act(make(place)), place))

    def each_source(make, places):
        for place in places:
            x, y = CIRCLE[place]
            pl.when(present(-x, -y))(functools.partial(lambda place: make(place).wait_recv(), place))

    def begin_copy(copy):
        copy.start()

    ways = range(len(WAYS))
    far = range(len(WAYS), len(CIRCLE))
    left = lax.broadcasted_iota(jnp.int32, (8, LANES), 1) < half

    hist[...] = jnp.zeros_like(hist)
    loads[0].wait()
    loads[1].wait()
    hist[0, 0:3, :] = start_ref[...]
    for pair in range(2):
        sidx[pair] = jnp.broadcast_to(
            jnp.concatenate(
                [sends_ref[2 * pair : 2 * pair + 1, :], sends_ref[2 * pair + 1 : 2 * pair + 2, :]],
                axis=1,
            ),
            (8, LANES),
        )

    def pack_w(turn, step):
        tables = [hist[step, :, tile(j)] for j in range(tiles)]
        picked = [pick(tables, sidx[pair], 0) for pair in range(2)]
        sendw[turn, 0] = jnp.concatenate([picked[0][0:4], picked[1][0:4]], axis=0)
        for j in range(0, tiles, 2):
            sendw[turn, 1 + j // 2] = jnp.concatenate([tables[j][0:4], tables[j + 1][0:4]], axis=0)

    pack_w(0, 0)

    loads[2].wait()
    loads[3].wait()
    agg = agg_ref[...]
    member = (
        jnp.broadcast_to(agg, (sizes_of, rows)) == lax.broadcasted_iota(jnp.int32, (sizes_of, rows), 0)
    ).astype(jnp.float32)
    counts = jnp.sum(member, axis=1, keepdims=True)
    sizes = jnp.sum(member * counts, axis=0, keepdims=True)
    tent = near_ref[...] * lax.rsqrt(sizes)
    tent_ref[...] = tent
    text[...] = jnp.zeros_like(text)
    for c in range(3):
        text[8 * c : 8 * c + modes, 0:rows] = tent_ref[modes * c : modes * (c + 1), :]
    for pair in range(2):
        for c in range(3):
            sendt[pair, 8 * c : 8 * c + 8, :] = pick(
                [text[8 * c : 8 * c + 8, tile(j)] for j in range(tiles)], sidx[pair], 0
            )

    loads[4].wait()
    loads[5].wait()
    rest_m[...] = jnp.zeros_like(rest_m)
    for u, places in enumerate(units):
        if len(places) * places[0][2] < 8:
            cols_u[u] = jnp.zeros((8, LANES), jnp.int32)
        for at, k, count, j in places:
            cols_u[u, at : at + count, :] = cols_ref[k : k + count, tile(j)]
            if count < 8:
                rest_m[planes - 1, j, 0:count, :] = cols_ref[k : k + count, tile(j)].astype(jnp.float32)

    inverse = invert_rows([diag_ref[p : p + 1, :] for p in range(9)])
    for p in range(9):
        dinv[p : p + 1, :] = inverse[p]
    pl.semaphore_wait(barrier, greeters)
    each_target(functools.partial(w_copy, 0), ORDER, begin_copy)
    loads[6].wait()
    for u, places in enumerate(units):
        if len(places) * places[0][2] < 8:
            mats[u] = jnp.zeros(mats.shape[1:], jnp.float32)
        for at, k, count, j in places:
            block = [off_v[p, k : k + count, tile(j)] for p in range(9)]
            for r in range(3):
                scale = [
                    jnp.broadcast_to(dinv[3 * r + q : 3 * r + q + 1, tile(j)], (count, LANES))
                    for q in range(3)
                ]
                for c in range(3):
                    entry = scale[0] * block[c] + scale[1] * block[3 + c] + scale[2] * block[6 + c]
                    mats[u, 3 * r + c, at : at + count, :] = entry
                    if count < 8:
                        rest_m[3 * r + c, j, 0:count, :] = entry

    def source(q, group, j):
        if 8 * (group + 1) > slots:
            return rest_m[q, j]
        u = group * tiles + j
        return cols_u[u].astype(jnp.float32) if q == planes - 1 else mats[u, q]

    def chosen(q, group, pair):
        if group >= groups:
            return jnp.zeros((8, LANES), jnp.float32)
        return pick([source(q, group, j) for j in range(tiles)], sidx[pair], 0)

    for pair in range(2):
        for v in range(gunits):
            for q in range(planes):
                low = chosen(q, 2 * v, pair)
                high = chosen(q, 2 * v + 1, pair)
                sendg[2 * pair, v, q] = jnp.where(left, low, pltpu.roll(high, half, 1))
                sendg[2 * pair + 1, v, q] = jnp.where(left, pltpu.roll(low, half, 1), high)
        each_target(g_copy, (2 * pair, 2 * pair + 1), begin_copy)
    each_target(t_copy, ways, begin_copy)

    per = -(-len(units) // (BLOCKS - 1))

    def spread(row):
        return jnp.broadcast_to(row, (8, LANES))

    def unit_products(u, unused):
        index = cols_u[u]
        for m in range(modes):
            picked = [
                pick(
                    [
                        spread(text[8 * c + m : 8 * c + m + 1, tile(i)])
                        for i in range(tiles + 2)
                    ],
                    index,
                    0,
                )
                for c in range(3)
            ]
            for r in range(3):
                raw_ref[modes * r + m, u] = (
                    mats[u, 3 * r] * picked[0]
                    + mats[u, 3 * r + 1] * picked[1]
                    + mats[u, 3 * r + 2] * picked[2]
                )
        return unused

    def contribute(tables, first, u):
        index = cols_u[u]
        picked = [pick(tables[c], index, first) for c in range(3)]
        return [sum(mats[u, 3 * r + c] * picked[c] for c in range(3)) for r in range(3)]

    def contribute_near(tables, first, way):
        total = [None] * 3
        for v in range(gunits):
            index = gcol[way, v]
            picked = [pick(tables[c], index, first) for c in range(3)]
            for r in range(3):
                term = sum(recvg[way, v, 3 * r + c] * picked[c] for c in range(3))
                total[r] = term if total[r] is None else total[r] + term
        return total

    def by_tile(terms):
        whole = [[None] * tiles for r in range(3)]
        for r in range(3):
            for u, places in enumerate(units):
                if len(places) == 1 and places[0][2] == 8:
                    j = places[0][3]
                    old = whole[r][j]
                    whole[r][j] = terms[u][r] if old is None else old + terms[u][r]
            for j in range(tiles):
                old = whole[r][j]
                whole[r][j] = 0.0 if old is None else jnp.sum(old, axis=0, keepdims=True)
            for u, places in enumerate(units):
                if not (len(places) == 1 and places[0][2] == 8):
                    for at, k, count, j in places:
                        whole[r][j] = whole[r][j] + jnp.sum(
                            terms[u][r][at : at + count], axis=0, keepdims=True
                        )
        return whole

    def own_part(step):
        tables = [[spread(hist[step, c : c + 1, tile(i)]) for i in range(tiles)] for c in range(3)]
        inner = by_tile([contribute(tables, 0, u) for u in range(len(units))])
        for r in range(3):
            for j in range(tiles):
                hist[step + 1, r : r + 1, tile(j)] = hist[step, r : r + 1, tile(j)] + inner[r][j]

    def ghost_part(step, tables):
        outer = by_tile([contribute(tables, tiles, u) for u in range(len(units))])
        for r in range(3):
            for j in range(tiles):
                hist[step + 1, r : r + 1, tile(j)] = hist[step + 1, r : r + 1, tile(j)] + outer[r][j]

    def halves(first, second, pair):
        both = jnp.where(left, first, second)
        return [both[4 * pair + c : 4 * pair + c + 1] for c in range(3)]

    def iterate(turn, unused):
        step = DEPTH * turn
        own_part(step)

        @pl.when(turn == 1)
        def _():
            each_source(t_copy, ways)
            for pair in range(2):
                for c in range(3):
                    text[8 * c : 8 * c + 8, tile(tiles + pair)] = jnp.where(
                        left,
                        recvt[2 * pair, 8 * c : 8 * c + 8, :],
                        recvt[2 * pair + 1, 8 * c : 8 * c + 8, :],
                    )

        lax.fori_loop(
            jnp.clip((turn - 1) * per, 0, len(units)), jnp.clip(turn * per, 0, len(units)), unit_products, 0
        )
        each_source(functools.partial(w_copy, turn), ways)
        merged = [
            halves(recvw[turn, 2 * pair, 0], recvw[turn, 2 * pair + 1, 0], pair) for pair in range(2)
        ]
        ghost_part(step, [[spread(merged[pair][c]) for pair in range(2)] for c in range(3)])

        @pl.when(turn == 0)
        def _():
            each_source(g_copy, ways)
            for way in ways:
                for v in range(gunits):
                    gcol[way, v] = recvg[way, v, planes - 1].astype(jnp.int32)

        inside = []
        for way in ways:
            tables = [
                [
                    spread(recvw[turn, way, 1 + i // 2, 4 * (i % 2) + c : 4 * (i % 2) + c + 1, :])
                    for i in range(tiles)
                ]
                for c in range(3)
            ]
            inside.append(contribute_near(tables, 0, way))
        own_part(step + 1)

        each_source(functools.partial(w_copy, turn), far)

        def packed(way, other):
            x, y = (WAYS[way][axis] + WAYS[other][axis] for axis in range(2))
            return sendw[turn, 0] if (x, y) == (0, 0) else recvp[turn, FAR.index((x, y))]

        total = []
        for way in ways:
            rows_of = [
                halves(packed(way, 2 * pair), packed(way, 2 * pair + 1), pair) for pair in range(2)
            ]
            outside = contribute_near(
                [[spread(rows_of[pair][c]) for pair in range(2)] for c in range(3)], tiles, way
            )
            total.append([inside[way][r] + outside[r] for r in range(3)])
        later = [[], [], []]
        for r in range(3):
            for pair in range(2):
                first, second = total[2 * pair][r], total[2 * pair + 1][r]
                both = jnp.where(left, first, second) + pltpu.roll(
                    jnp.where(left, second, first), half, 1
                )
                later[r].append(spread(merged[pair][r] + jnp.sum(both, axis=0, keepdims=True)))
        ghost_part(step + 1, later)

        @pl.when(turn < BLOCKS - 1)
        def _():
            pack_w(turn + 1, step + DEPTH)
            each_target(functools.partial(w_copy, turn + 1), ORDER, begin_copy)

        return unused

    lax.fori_loop(0, BLOCKS, iterate, 0)

    def squares(t):
        return jnp.sum(
            sum(hist[t, :, tile(j)] * hist[t, :, tile(j)] for j in range(tiles)), keepdims=True
        )

    lane = lax.broadcasted_iota(jnp.int32, (1, LANES), 1)
    latest = jnp.broadcast_to(squares(ITERS), (1, LANES))
    previous = jnp.broadcast_to(squares(ITERS - 1), (1, LANES))
    own = jnp.where(lane == 0, latest, jnp.where(lane == 1, previous, 0.0))
    me = a * n_sub + b
    devices = n_slab * n_sub
    stat[0] = own

    def stat_copy(step, source):
        target = lax.rem(me + step, devices)
        landing = lax.rem(me + devices - step, devices) if source else me
        return pltpu.make_async_remote_copy(
            src_ref=stat.at[0], dst_ref=stats.at[landing],
            send_sem=ss_sem.at[step], recv_sem=rs_sem.at[landing],
            device_id={"slab": lax.div(target, n_sub), "sub": lax.rem(target, n_sub)},
            device_id_type=MESH,
        )

    def begin(step, unused):
        stat_copy(step, False).start()
        return unused

    def arrive(step, unused):
        stat_copy(step, True).wait_recv()
        return unused

    def sent(step, unused):
        stat_copy(step, False).wait_send()
        return unused

    lax.fori_loop(1, devices, begin, 0)
    stats[me] = own
    lax.fori_loop(1, devices, arrive, 0)
    whole = jnp.sum(stats[...], axis=0)
    latest = whole[:, 0:1]
    previous = whole[:, 1:2]
    rho_ref[...] = jnp.sqrt(latest / (previous + 1e-05))

    lax.fori_loop(1, devices, sent, 0)
    def settle(copy):
        copy.wait_send()

    each_target(g_copy, ways, settle)
    each_target(t_copy, ways, settle)

    def drain(turn, unused):
        each_target(functools.partial(w_copy, turn), ORDER, settle)
        return unused

    lax.fori_loop(0, BLOCKS, drain, 0)


def body(n_slab, n_sub, near_null, aggregates, diag_block, off_blocks, columns, sends, start_vector):
    slots, nine, rows = off_blocks.shape
    wide = rows + 2 * LANES
    count = len(unit_places(slots, rows // LANES))
    parts = 1 + rows // (2 * LANES)
    gunits = -(-slots // 16)
    f32 = jnp.float32
    vmem = pl.BlockSpec(memory_space=pltpu.VMEM)
    dma = pltpu.SemaphoreType.DMA
    raw, tentative, rho = pl.pallas_call(
        functools.partial(kernel, n_slab, n_sub),
        out_shape=(
            pltpu.VMEM((near_null.shape[0], count, 8, LANES), f32),
            pltpu.VMEM(near_null.shape, f32),
            jax.ShapeDtypeStruct((1, 1), f32),
        ),
        in_specs=[pl.BlockSpec(memory_space=pltpu.HBM)] * 7,
        out_specs=(vmem, vmem, vmem),
        scratch_shapes=[
            pltpu.VMEM(near_null.shape, f32),
            pltpu.VMEM((1, rows), jnp.int32),
            pltpu.VMEM(diag_block.shape, f32),
            pltpu.VMEM(columns.shape, jnp.int32),
            pltpu.VMEM(sends.shape, jnp.int32),
            pltpu.VMEM(start_vector.shape, f32),
            pltpu.VMEM((nine, slots, rows), f32),
            pltpu.VMEM((count, 8, LANES), jnp.int32),
            pltpu.VMEM((count, nine, 8, LANES), f32),
            pltpu.VMEM((nine + 1, rows // LANES, 8, LANES), f32),
            pltpu.VMEM((16, rows), f32),
            pltpu.VMEM((24, wide), f32),
            pltpu.VMEM((ITERS + 1, 8, rows), f32),
            pltpu.VMEM((2, 8, LANES), jnp.int32),
            pltpu.VMEM((BLOCKS, parts, 8, LANES), f32),
            pltpu.VMEM((BLOCKS, len(WAYS), parts, 8, LANES), f32),
            pltpu.VMEM((BLOCKS, len(FAR), 8, LANES), f32),
            pltpu.VMEM((len(WAYS), gunits, nine + 1, 8, LANES), f32),
            pltpu.VMEM((len(WAYS), gunits, nine + 1, 8, LANES), f32),
            pltpu.VMEM((len(WAYS), gunits, 8, LANES), jnp.int32),
            pltpu.VMEM((2, 24, LANES), f32),
            pltpu.VMEM((4, 24, LANES), f32),
            pltpu.VMEM((1, 1, LANES), f32),
            pltpu.VMEM((n_slab * n_sub, 1, LANES), f32),
            dma((7,)),
            dma((BLOCKS, len(CIRCLE))),
            dma((BLOCKS, len(CIRCLE))),
            dma((4,)),
            dma((4,)),
            dma((4,)),
            dma((4,)),
            dma((n_slab * n_sub,)),
            dma((n_slab * n_sub,)),
        ],
        compiler_params=pltpu.CompilerParams(collective_id=0, has_side_effects=True, vmem_limit_bytes=16777216),
        name="smooth",
    )(
        *[
            pltpu.with_memory_space_constraint(x, pltpu.HBM)
            for x in (
                near_null, aggregates.reshape(1, rows), diag_block, off_blocks.transpose(1, 0, 2),
                columns, sends, start_vector,
            )
        ]
    )
    prolong_off, prolong_self, rho = pl.pallas_call(
        scale_kernel,
        out_shape=(
            jax.ShapeDtypeStruct((near_null.shape[0], slots, rows), jnp.bfloat16),
            jax.ShapeDtypeStruct(near_null.shape, jnp.bfloat16),
            jax.ShapeDtypeStruct((1, 1), f32),
        ),
        in_specs=[vmem, vmem, vmem],
        out_specs=(vmem, vmem, vmem),
        compiler_params=pltpu.CompilerParams(vmem_limit_bytes=16777216),
        name="scale",
    )(raw, tentative, rho)
    return (prolong_off.transpose(1, 0, 2), prolong_self, rho.reshape(()))


def solution(mesh):
    placed = (
        P(None, ("slab", "sub")),
        P(("slab", "sub")),
        P(None, ("slab", "sub")),
        P(None, None, ("slab", "sub")),
        P(None, ("slab", "sub")),
        P(None, ("slab", "sub")),
        P(None, ("slab", "sub")),
    )
    return jax.shard_map(
        functools.partial(body, mesh.shape["slab"], mesh.shape["sub"]),
        mesh=mesh,
        in_specs=placed,
        out_specs=(P(None, None, ("slab", "sub")), P(None, ("slab", "sub")), P()),
        check_vma=False,
    )
```

```python
import functools

import jax
import jax.numpy as jnp
from jax import lax
from jax.experimental import pallas as pl
from jax.experimental.pallas import tpu as pltpu
from jax.sharding import PartitionSpec as P

ITERS = 8
OMEGA = 4.0 / 3.0
LANES = 128
MESH = pl.DeviceIdType.MESH
LOAD_ORDER = [0, 1, 4, 5, 2, 3]
DEPTH = 2
BLOCKS = ITERS // DEPTH
WAYS = [(0, 1), (0, -1), (1, 0), (-1, 0)]
FAR = [(-1, -1), (-1, 1), (1, -1), (1, 1), (-2, 0), (2, 0), (0, -2), (0, 2)]
CIRCLE = WAYS + FAR
ORDER = list(range(len(WAYS), len(CIRCLE))) + list(range(len(WAYS)))


def lane_gather(table, lanes):
    return jnp.take_along_axis(table, lanes, axis=1, mode="promise_in_bounds")


def tile(number):
    return pl.ds(number * LANES, LANES)


def pick(tables, index, first):
    high = index >> 7
    low = index & (LANES - 1)
    out = jnp.zeros(index.shape, jnp.float32)
    for step, table in enumerate(tables):
        out = jnp.where(high == first + step, lane_gather(table, low), out)
    return out


def invert_rows(entries):
    cofactor = [
        entries[4] * entries[8] - entries[5] * entries[7],
        entries[5] * entries[6] - entries[3] * entries[8],
        entries[3] * entries[7] - entries[4] * entries[6],
        entries[2] * entries[7] - entries[1] * entries[8],
        entries[0] * entries[8] - entries[2] * entries[6],
        entries[1] * entries[6] - entries[0] * entries[7],
        entries[1] * entries[5] - entries[2] * entries[4],
        entries[2] * entries[3] - entries[0] * entries[5],
        entries[0] * entries[4] - entries[1] * entries[3],
    ]
    determinant = entries[0] * cofactor[0] + entries[1] * cofactor[1] + entries[2] * cofactor[2]
    return [
        cofactor[column * 3 + row] / determinant for row in range(3) for column in range(3)
    ]


def unit_places(slots, tiles):
    units = []
    for k in range(0, slots - 7, 8):
        for j in range(tiles):
            units.append([(0, k, 8, j)])
    rest = slots % 8
    if rest:
        share = 8 // rest
        for j in range(0, tiles, share):
            units.append(
                [
                    (rest * i, slots - rest, rest, j + i)
                    for i in range(min(share, tiles - j))
                ]
            )
    return units


def scale_kernel(raw_ref, tent_ref, rho_ref, off_ref, self_ref, out_rho_ref):
    slots, rows = off_ref.shape[1:]
    out_rho_ref[...] = rho_ref[...]
    inverse = OMEGA / rho_ref[...]
    factor = jnp.broadcast_to(-inverse, (8, LANES))
    places = unit_places(slots, rows // LANES)
    for j in range(rows // LANES):
        for entry in range(off_ref.shape[0]):
            parts = [
                (raw_ref[entry, u] * factor)[at : at + count]
                for u in range(len(places))
                for at, k, count, tile_number in places[u]
                if tile_number == j
            ]
            off_ref[entry, :, tile(j)] = jnp.concatenate(parts, axis=0).astype(off_ref.dtype)
    self_ref[...] = ((1.0 - inverse) * tent_ref[...]).astype(self_ref.dtype)


def kernel(
    n_slab, n_sub,
    near_hbm, agg_hbm, diag_hbm, off_hbm, cols_hbm, sends_hbm, start_hbm,
    raw_ref, tent_ref, rho_ref,
    near_ref, agg_ref, diag_ref, cols_ref, sends_ref, start_ref, off_v, cols_u, mats, rest_m, dinv, text, hist, sidx,
    sendw, recvw, sendu, recvu, sendg, recvg, gcol, sendt, recvt, stat, stats,
    off_sem, sendw_sem, recvw_sem, sendu_sem, recvu_sem, sendg_sem, recvg_sem, sendt_sem, recvt_sem,
    ss_sem, rs_sem,
):
    slots, rows = cols_ref.shape
    half = sends_ref.shape[1]
    tiles = rows // LANES
    units = unit_places(slots, tiles)
    groups = -(-slots // 8)
    gunits, planes = sendg.shape[1:3]
    modes = near_ref.shape[0] // 3
    sizes_of = rows // 8
    a = lax.axis_index("slab")
    b = lax.axis_index("sub")
    barrier = pltpu.get_barrier_semaphore()
    def present(x, y):
        return (a + x >= 0) & (a + x < n_slab) & (b + y >= 0) & (b + y < n_sub)

    def greet(x, y):
        pl.semaphore_signal(
            barrier, inc=1, device_id={"slab": a + x, "sub": b + y}, device_id_type=MESH
        )

    def greet_any(step, unused):
        target = lax.rem(a * n_sub + b + step, n_slab * n_sub)
        greet(lax.div(target, n_sub) - a, lax.rem(target, n_sub) - b)
        return unused

    near = n_slab - 1 + n_sub - 1 <= ITERS + 2
    if near:
        for x, y in CIRCLE:
            pl.when(present(x, y))(functools.partial(greet, x, y))
        greeters = sum(present(x, y).astype(jnp.int32) for x, y in CIRCLE)
    else:
        lax.fori_loop(1, n_slab * n_sub, greet_any, 0)
        greeters = n_slab * n_sub - 1

    loads = [
        pltpu.make_async_copy(source, target, off_sem.at[number])
        for number, (source, target) in enumerate(
            (
                (start_hbm, start_ref),
                (sends_hbm, sends_ref),
                (agg_hbm, agg_ref),
                (near_hbm, near_ref),
                (diag_hbm, diag_ref),
                (cols_hbm, cols_ref),
            )
        )
    ]
    cuts = [(16 * v, min(16, slots - 16 * v)) for v in range(gunits)]
    loads += [
        pltpu.make_async_copy(
            off_hbm.at[:, pl.ds(k, count)], off_v.at[:, pl.ds(k, count)], off_sem.at[len(loads) + v]
        )
        for v, (k, count) in enumerate(cuts)
    ]
    for number in LOAD_ORDER + list(range(len(LOAD_ORDER), len(loads))):
        loads[number].start()

    def clear(place):
        cleared = [recvw.at[:, place]]
        if place < len(WAYS):
            cleared += [recvu.at[:, place], recvg.at[place], recvt.at[place]]
        for ref in cleared:
            ref[...] = jnp.zeros(ref.shape, jnp.float32)

    for place, (x, y) in enumerate(CIRCLE):
        pl.when(jnp.logical_not(present(-x, -y)))(functools.partial(clear, place))

    def remote(source, target, sent, came, place):
        x, y = CIRCLE[place]
        return pltpu.make_async_remote_copy(
            src_ref=source, dst_ref=target, send_sem=sent, recv_sem=came,
            device_id={"slab": a + x, "sub": b + y}, device_id_type=MESH,
        )

    def w_copy(turn, place):
        return remote(
            sendw.at[turn], recvw.at[turn, place],
            sendw_sem.at[place], recvw_sem.at[lax.rem(turn, 2), place], place,
        )

    def u_copy(turn, way):
        return remote(
            sendu.at[turn], recvu.at[turn, way],
            sendu_sem.at[way], recvu_sem.at[lax.rem(turn, 2), way], way,
        )

    def g_copy(v, way):
        return remote(
            sendg.at[way, v], recvg.at[way, v], sendg_sem.at[way], recvg_sem.at[way], way
        )

    def g_whole(way):
        return remote(sendg.at[way], recvg.at[way], sendg_sem.at[way], recvg_sem.at[way], way)

    def t_copy(way):
        return remote(sendt.at[way // 2], recvt.at[way], sendt_sem.at[way], recvt_sem.at[way], way)

    def each_target(make, places, act):
        for place in places:
            x, y = CIRCLE[place]
            pl.when(present(x, y))(functools.partial(lambda place: act(make(place)), place))

    def each_source(make, places):
        for place in places:
            x, y = CIRCLE[place]
            pl.when(present(-x, -y))(functools.partial(lambda place: make(place).wait_recv(), place))

    def begin_copy(copy):
        copy.start()

    def settle(copy):
        copy.wait_send()

    ways = range(len(WAYS))
    far = range(len(WAYS), len(CIRCLE))
    left = lax.broadcasted_iota(jnp.int32, (8, LANES), 1) < half

    hist[...] = jnp.zeros_like(hist)
    loads[0].wait()
    loads[1].wait()
    hist[0, 0:3, :] = start_ref[...]
    for pair in range(2):
        sidx[pair] = jnp.broadcast_to(
            jnp.concatenate(
                [sends_ref[2 * pair : 2 * pair + 1, :], sends_ref[2 * pair + 1 : 2 * pair + 2, :]],
                axis=1,
            ),
            (8, LANES),
        )

    def listed(step):
        tables = [hist[step, :, tile(j)] for j in range(tiles)]
        picked = [pick(tables, sidx[pair], 0) for pair in range(2)]
        return jnp.concatenate([picked[0][0:4], picked[1][0:4]], axis=0)

    sendw[0] = listed(0)

    loads[4].wait()
    loads[5].wait()
    inverse = invert_rows([diag_ref[p : p + 1, :] for p in range(9)])
    for p in range(9):
        dinv[p : p + 1, :] = inverse[p]
    rest_m[...] = jnp.zeros_like(rest_m)
    for u, places in enumerate(units):
        if len(places) * places[0][2] < 8:
            cols_u[u] = jnp.zeros((8, LANES), jnp.int32)
        for at, k, count, j in places:
            cols_u[u, at : at + count, :] = cols_ref[k : k + count, tile(j)]
            if count < 8:
                rest_m[planes - 1, j, 0:count, :] = cols_ref[k : k + count, tile(j)].astype(jnp.float32)

    def source(q, group, j):
        if 8 * (group + 1) > slots:
            return rest_m[q, j]
        u = group * tiles + j
        return cols_u[u].astype(jnp.float32) if q == planes - 1 else mats[u, q]

    def chosen(q, group, pair):
        if group >= groups:
            return jnp.zeros((8, LANES), jnp.float32)
        return pick([source(q, group, j) for j in range(tiles)], sidx[pair], 0)

    for v, (cut, length) in enumerate(cuts):
        loads[6 + v].wait()
        for u, places in enumerate(units):
            if not cut <= places[0][1] < cut + length:
                continue
            if len(places) * places[0][2] < 8:
                mats[u] = jnp.zeros(mats.shape[1:], jnp.float32)
            for at, k, count, j in places:
                block = [off_v[p, k : k + count, tile(j)] for p in range(9)]
                for r in range(3):
                    scale = [
                        jnp.broadcast_to(dinv[3 * r + q : 3 * r + q + 1, tile(j)], (count, LANES))
                        for q in range(3)
                    ]
                    for c in range(3):
                        entry = scale[0] * block[c] + scale[1] * block[3 + c] + scale[2] * block[6 + c]
                        mats[u, 3 * r + c, at : at + count, :] = entry
                        if count < 8:
                            rest_m[3 * r + c, j, 0:count, :] = entry
        for pair in (1, 0):
            for q in range(planes):
                low = chosen(q, 2 * v, pair)
                high = chosen(q, 2 * v + 1, pair)
                sendg[2 * pair, v, q] = jnp.where(left, low, pltpu.roll(high, half, 1))
                sendg[2 * pair + 1, v, q] = jnp.where(left, pltpu.roll(low, half, 1), high)
            if v == 0 and pair == 1:
                pl.semaphore_wait(barrier, greeters)
                each_target(functools.partial(w_copy, 0), ORDER, begin_copy)
            each_target(functools.partial(g_copy, v), (2 * pair, 2 * pair + 1), begin_copy)

    def tentative():
        loads[2].wait()
        loads[3].wait()
        agg = agg_ref[...]
        member = (
            jnp.broadcast_to(agg, (sizes_of, rows)) == lax.broadcasted_iota(jnp.int32, (sizes_of, rows), 0)
        ).astype(jnp.float32)
        counts = jnp.sum(member, axis=1, keepdims=True)
        sizes = jnp.sum(member * counts, axis=0, keepdims=True)
        tent_ref[...] = near_ref[...] * lax.rsqrt(sizes)
        text[...] = jnp.zeros_like(text)
        for c in range(3):
            text[8 * c : 8 * c + modes, 0:rows] = tent_ref[modes * c : modes * (c + 1), :]
        for pair in range(2):
            for c in range(3):
                sendt[pair, 8 * c : 8 * c + 8, :] = pick(
                    [text[8 * c : 8 * c + 8, tile(j)] for j in range(tiles)], sidx[pair], 0
                )
        each_target(t_copy, ways, begin_copy)

    per = -(-len(units) // (BLOCKS - 1))

    def spread(row):
        return jnp.broadcast_to(row, (8, LANES))

    def unit_products(u, unused):
        index = cols_u[u]
        for m in range(modes):
            picked = [
                pick(
                    [
                        spread(text[8 * c + m : 8 * c + m + 1, tile(i)])
                        for i in range(tiles + 2)
                    ],
                    index,
                    0,
                )
                for c in range(3)
            ]
            for r in range(3):
                raw_ref[modes * r + m, u] = (
                    mats[u, 3 * r] * picked[0]
                    + mats[u, 3 * r + 1] * picked[1]
                    + mats[u, 3 * r + 2] * picked[2]
                )
        return unused

    def contribute(tables, first, u):
        index = cols_u[u]
        picked = [pick(tables[c], index, first) for c in range(3)]
        return [sum(mats[u, 3 * r + c] * picked[c] for c in range(3)) for r in range(3)]

    def contribute_near(tables, first, way):
        total = [None] * 3
        for v in range(gunits):
            index = gcol[way, v]
            picked = [pick(tables[c], index, first) for c in range(3)]
            for r in range(3):
                term = sum(recvg[way, v, 3 * r + c] * picked[c] for c in range(3))
                total[r] = term if total[r] is None else total[r] + term
        return total

    def by_tile(terms):
        whole = [[None] * tiles for r in range(3)]
        for r in range(3):
            for u, places in enumerate(units):
                if len(places) == 1 and places[0][2] == 8:
                    j = places[0][3]
                    old = whole[r][j]
                    whole[r][j] = terms[u][r] if old is None else old + terms[u][r]
            for j in range(tiles):
                old = whole[r][j]
                whole[r][j] = 0.0 if old is None else jnp.sum(old, axis=0, keepdims=True)
            for u, places in enumerate(units):
                if not (len(places) == 1 and places[0][2] == 8):
                    for at, k, count, j in places:
                        whole[r][j] = whole[r][j] + jnp.sum(
                            terms[u][r][at : at + count], axis=0, keepdims=True
                        )
        return whole

    def own_part(step):
        tables = [[spread(hist[step, c : c + 1, tile(i)]) for i in range(tiles)] for c in range(3)]
        inner = by_tile([contribute(tables, 0, u) for u in range(len(units))])
        for r in range(3):
            for j in range(tiles):
                hist[step + 1, r : r + 1, tile(j)] = hist[step, r : r + 1, tile(j)] + inner[r][j]

    def ghost_part(step, tables):
        outer = by_tile([contribute(tables, tiles, u) for u in range(len(units))])
        for r in range(3):
            for j in range(tiles):
                hist[step + 1, r : r + 1, tile(j)] = hist[step + 1, r : r + 1, tile(j)] + outer[r][j]

    def halves(first, second, pair):
        both = jnp.where(left, first, second)
        return [both[4 * pair + c : 4 * pair + c + 1] for c in range(3)]

    def iterate(turn, unused):
        step = DEPTH * turn
        own_part(step)
        sendu[turn] = listed(step + 1)
        each_target(functools.partial(u_copy, turn), ways, begin_copy)
        pl.when(turn == 0)(tentative)

        @pl.when(turn == 1)
        def _():
            each_source(t_copy, ways)
            for pair in range(2):
                for c in range(3):
                    text[8 * c : 8 * c + 8, tile(tiles + pair)] = jnp.where(
                        left,
                        recvt[2 * pair, 8 * c : 8 * c + 8, :],
                        recvt[2 * pair + 1, 8 * c : 8 * c + 8, :],
                    )

        lax.fori_loop(
            jnp.clip((turn - 1) * per, 0, len(units)), jnp.clip(turn * per, 0, len(units)), unit_products, 0
        )
        each_target(functools.partial(w_copy, turn), ORDER, settle)
        each_target(functools.partial(u_copy, turn), ways, settle)
        each_source(functools.partial(w_copy, turn), ways)
        merged = [halves(recvw[turn, 2 * pair], recvw[turn, 2 * pair + 1], pair) for pair in range(2)]
        ghost_part(step, [[spread(merged[pair][c]) for pair in range(2)] for c in range(3)])
        own_part(step + 1)

        @pl.when(turn == 0)
        def _():
            each_source(g_whole, ways)
            for way in ways:
                for v in range(gunits):
                    gcol[way, v] = recvg[way, v, planes - 1].astype(jnp.int32)

        each_source(functools.partial(w_copy, turn), far)

        def packed(way, other):
            x, y = (WAYS[way][axis] + WAYS[other][axis] for axis in range(2))
            return sendw[turn] if (x, y) == (0, 0) else recvw[turn, CIRCLE.index((x, y))]

        total = []
        for way in ways:
            rows_of = [
                halves(packed(way, 2 * pair), packed(way, 2 * pair + 1), pair) for pair in range(2)
            ]
            total.append(
                contribute_near(
                    [[spread(rows_of[pair][c]) for pair in range(2)] for c in range(3)], tiles, way
                )
            )
        each_source(functools.partial(u_copy, turn), ways)
        base = [halves(recvu[turn, 2 * pair], recvu[turn, 2 * pair + 1], pair) for pair in range(2)]
        later = [[], [], []]
        for r in range(3):
            for pair in range(2):
                first, second = total[2 * pair][r], total[2 * pair + 1][r]
                both = jnp.where(left, first, second) + pltpu.roll(
                    jnp.where(left, second, first), half, 1
                )
                later[r].append(spread(base[pair][r] + jnp.sum(both, axis=0, keepdims=True)))
        ghost_part(step + 1, later)

        @pl.when(turn < BLOCKS - 1)
        def _():
            sendw[turn + 1] = listed(step + DEPTH)
            each_target(functools.partial(w_copy, turn + 1), ORDER, begin_copy)

        return unused

    lax.fori_loop(0, BLOCKS, iterate, 0)

    def squares(t):
        return jnp.sum(
            sum(hist[t, :, tile(j)] * hist[t, :, tile(j)] for j in range(tiles)), keepdims=True
        )

    lane = lax.broadcasted_iota(jnp.int32, (1, LANES), 1)
    latest = jnp.broadcast_to(squares(ITERS), (1, LANES))
    previous = jnp.broadcast_to(squares(ITERS - 1), (1, LANES))
    own = jnp.where(lane == 0, latest, jnp.where(lane == 1, previous, 0.0))
    me = a * n_sub + b
    devices = n_slab * n_sub
    stat[0] = own

    def begin(step, unused):
        target = lax.rem(me + jnp.where(2 * a < n_slab, devices - step, step), devices)
        pltpu.make_async_remote_copy(
            src_ref=stat.at[0], dst_ref=stats.at[me], send_sem=ss_sem, recv_sem=rs_sem,
            device_id={"slab": lax.div(target, n_sub), "sub": lax.rem(target, n_sub)},
            device_id_type=MESH,
        ).start()
        return unused

    lax.fori_loop(1, devices, begin, 0)
    stats[me] = own
    others = stats.at[pl.ds(0, devices - 1)]
    everything = pltpu.make_async_remote_copy(
        src_ref=others, dst_ref=others, send_sem=ss_sem, recv_sem=rs_sem,
        device_id={"slab": n_slab - 1 - a, "sub": n_sub - 1 - b}, device_id_type=MESH,
    )
    everything.wait_recv()
    whole = jnp.sum(stats[...], axis=0)
    latest = whole[:, 0:1]
    previous = whole[:, 1:2]
    rho_ref[...] = jnp.sqrt(latest / (previous + 1e-05))

    everything.wait_send()
    each_target(g_whole, ways, settle)
    each_target(t_copy, ways, settle)


def body(n_slab, n_sub, near_null, aggregates, diag_block, off_blocks, columns, sends, start_vector):
    slots, nine, rows = off_blocks.shape
    wide = rows + 2 * LANES
    count = len(unit_places(slots, rows // LANES))
    gunits = -(-slots // 16)
    f32 = jnp.float32
    vmem = pl.BlockSpec(memory_space=pltpu.VMEM)
    dma = pltpu.SemaphoreType.DMA
    raw, tentative, rho = pl.pallas_call(
        functools.partial(kernel, n_slab, n_sub),
        out_shape=(
            pltpu.VMEM((near_null.shape[0], count, 8, LANES), f32),
            pltpu.VMEM(near_null.shape, f32),
            jax.ShapeDtypeStruct((1, 1), f32),
        ),
        in_specs=[pl.BlockSpec(memory_space=pltpu.HBM)] * 7,
        out_specs=(vmem, vmem, vmem),
        scratch_shapes=[
            pltpu.VMEM(near_null.shape, f32),
            pltpu.VMEM((1, rows), jnp.int32),
            pltpu.VMEM(diag_block.shape, f32),
            pltpu.VMEM(columns.shape, jnp.int32),
            pltpu.VMEM(sends.shape, jnp.int32),
            pltpu.VMEM(start_vector.shape, f32),
            pltpu.VMEM((nine, slots, rows), f32),
            pltpu.VMEM((count, 8, LANES), jnp.int32),
            pltpu.VMEM((count, nine, 8, LANES), f32),
            pltpu.VMEM((nine + 1, rows // LANES, 8, LANES), f32),
            pltpu.VMEM((16, rows), f32),
            pltpu.VMEM((24, wide), f32),
            pltpu.VMEM((ITERS + 1, 8, rows), f32),
            pltpu.VMEM((2, 8, LANES), jnp.int32),
            pltpu.VMEM((BLOCKS, 8, LANES), f32),
            pltpu.VMEM((BLOCKS, len(CIRCLE), 8, LANES), f32),
            pltpu.VMEM((BLOCKS, 8, LANES), f32),
            pltpu.VMEM((BLOCKS, len(WAYS), 8, LANES), f32),
            pltpu.VMEM((len(WAYS), gunits, nine + 1, 8, LANES), f32),
            pltpu.VMEM((len(WAYS), gunits, nine + 1, 8, LANES), f32),
            pltpu.VMEM((len(WAYS), gunits, 8, LANES), jnp.int32),
            pltpu.VMEM((2, 24, LANES), f32),
            pltpu.VMEM((4, 24, LANES), f32),
            pltpu.VMEM((1, 1, LANES), f32),
            pltpu.VMEM((n_slab * n_sub, 1, LANES), f32),
            dma((6 + gunits,)),
            dma((len(CIRCLE),)),
            dma((2, len(CIRCLE))),
            dma((len(WAYS),)),
            dma((2, len(WAYS))),
            dma((len(WAYS),)),
            dma((len(WAYS),)),
            dma((len(WAYS),)),
            dma((len(WAYS),)),
            dma,
            dma,
        ],
        compiler_params=pltpu.CompilerParams(collective_id=0, has_side_effects=True, vmem_limit_bytes=16777216),
        name="smooth",
    )(
        *[
            pltpu.with_memory_space_constraint(x, pltpu.HBM)
            for x in (
                near_null, aggregates.reshape(1, rows), diag_block, off_blocks.transpose(1, 0, 2),
                columns, sends, start_vector,
            )
        ]
    )
    prolong_off, prolong_self, rho = pl.pallas_call(
        scale_kernel,
        out_shape=(
            jax.ShapeDtypeStruct((near_null.shape[0], slots, rows), jnp.bfloat16),
            jax.ShapeDtypeStruct(near_null.shape, jnp.bfloat16),
            jax.ShapeDtypeStruct((1, 1), f32),
        ),
        in_specs=[vmem, vmem, vmem],
        out_specs=(vmem, vmem, vmem),
        compiler_params=pltpu.CompilerParams(vmem_limit_bytes=16777216),
        name="scale",
    )(raw, tentative, rho)
    return (prolong_off.transpose(1, 0, 2), prolong_self, rho.reshape(()))


def solution(mesh):
    placed = (
        P(None, ("slab", "sub")),
        P(("slab", "sub")),
        P(None, ("slab", "sub")),
        P(None, None, ("slab", "sub")),
        P(None, ("slab", "sub")),
        P(None, ("slab", "sub")),
        P(None, ("slab", "sub")),
    )
    return jax.shard_map(
        functools.partial(body, mesh.shape["slab"], mesh.shape["sub"]),
        mesh=mesh,
        in_specs=placed,
        out_specs=(P(None, None, ("slab", "sub")), P(None, ("slab", "sub")), P()),
        check_vma=False,
    )
```

```python
import functools

import jax
import jax.numpy as jnp
from jax import lax
from jax.experimental import pallas as pl
from jax.experimental.pallas import tpu as pltpu
from jax.sharding import PartitionSpec as P

ITERS = 8
OMEGA = 4.0 / 3.0
LANES = 128
MESH = pl.DeviceIdType.MESH
LOAD_ORDER = [0, 1, 4, 5, 2, 3]
DEPTH = 2
BLOCKS = ITERS // DEPTH
WAYS = [(0, 1), (0, -1), (1, 0), (-1, 0)]
FAR = [(-1, -1), (-1, 1), (1, -1), (1, 1), (-2, 0), (2, 0), (0, -2), (0, 2)]
CIRCLE = WAYS + FAR
ORDER = list(range(len(WAYS), len(CIRCLE))) + list(range(len(WAYS)))


def lane_gather(table, lanes):
    return jnp.take_along_axis(table, lanes, axis=1, mode="promise_in_bounds")


def tile(number):
    return pl.ds(number * LANES, LANES)


def pick(tables, index, first):
    high = index >> 7
    low = index & (LANES - 1)
    out = jnp.zeros(index.shape, jnp.float32)
    for step, table in enumerate(tables):
        out = jnp.where(high == first + step, lane_gather(table, low), out)
    return out


def invert_rows(entries):
    cofactor = [
        entries[4] * entries[8] - entries[5] * entries[7],
        entries[5] * entries[6] - entries[3] * entries[8],
        entries[3] * entries[7] - entries[4] * entries[6],
        entries[2] * entries[7] - entries[1] * entries[8],
        entries[0] * entries[8] - entries[2] * entries[6],
        entries[1] * entries[6] - entries[0] * entries[7],
        entries[1] * entries[5] - entries[2] * entries[4],
        entries[2] * entries[3] - entries[0] * entries[5],
        entries[0] * entries[4] - entries[1] * entries[3],
    ]
    determinant = entries[0] * cofactor[0] + entries[1] * cofactor[1] + entries[2] * cofactor[2]
    return [
        cofactor[column * 3 + row] / determinant for row in range(3) for column in range(3)
    ]


def unit_places(slots, tiles):
    units = []
    for k in range(0, slots - 7, 8):
        for j in range(tiles):
            units.append([(0, k, 8, j)])
    rest = slots % 8
    if rest:
        share = 8 // rest
        for j in range(0, tiles, share):
            units.append(
                [
                    (rest * i, slots - rest, rest, j + i)
                    for i in range(min(share, tiles - j))
                ]
            )
    return units


def scale_kernel(raw_ref, tent_ref, rho_ref, off_ref, self_ref, out_rho_ref):
    slots, rows = off_ref.shape[1:]
    out_rho_ref[...] = rho_ref[...]
    inverse = OMEGA / rho_ref[...]
    factor = jnp.broadcast_to(-inverse, (8, LANES))
    places = unit_places(slots, rows // LANES)
    for j in range(rows // LANES):
        for entry in range(off_ref.shape[0]):
            parts = [
                (raw_ref[entry, u] * factor)[at : at + count]
                for u in range(len(places))
                for at, k, count, tile_number in places[u]
                if tile_number == j
            ]
            off_ref[entry, :, tile(j)] = jnp.concatenate(parts, axis=0).astype(off_ref.dtype)
    self_ref[...] = ((1.0 - inverse) * tent_ref[...]).astype(self_ref.dtype)


def kernel(
    n_slab, n_sub,
    near_hbm, agg_hbm, diag_hbm, off_hbm, cols_hbm, sends_hbm, start_hbm,
    raw_ref, tent_ref, rho_ref,
    near_ref, agg_ref, diag_ref, cols_ref, sends_ref, start_ref, off_v, cols_u, mats, rest_m, dinv, text, hist, sidx,
    sendw, recvw, sendu, recvu, mine, minecol, sendg, recvg, gcol, sendt, recvt, stat, stats,
    ss_sem, rs_sem,
):
    a = lax.axis_index("slab")
    b = lax.axis_index("sub")
    devices = n_slab * n_sub

    def power(
        off_sem, sendw_sem, recvw_sem, sendu_sem, recvu_sem, sendg_sem, recvg_sem, sendt_sem, recvt_sem
    ):
        slots, rows = cols_ref.shape
        half = sends_ref.shape[1]
        tiles = rows // LANES
        units = unit_places(slots, tiles)
        groups = -(-slots // 8)
        gunits, planes = sendg.shape[1:3]
        modes = near_ref.shape[0] // 3
        sizes_of = rows // 8
        barrier = pltpu.get_barrier_semaphore()
        def present(x, y):
            return (a + x >= 0) & (a + x < n_slab) & (b + y >= 0) & (b + y < n_sub)

        def greet(x, y):
            pl.semaphore_signal(
                barrier, inc=1, device_id={"slab": a + x, "sub": b + y}, device_id_type=MESH
            )

        def greet_any(step, unused):
            target = lax.rem(a * n_sub + b + step, n_slab * n_sub)
            greet(lax.div(target, n_sub) - a, lax.rem(target, n_sub) - b)
            return unused

        near = n_slab - 1 + n_sub - 1 <= ITERS + 2
        if near:
            for x, y in CIRCLE:
                pl.when(present(x, y))(functools.partial(greet, x, y))
            greeters = sum(present(x, y).astype(jnp.int32) for x, y in CIRCLE)
        else:
            lax.fori_loop(1, n_slab * n_sub, greet_any, 0)
            greeters = n_slab * n_sub - 1

        loads = [
            pltpu.make_async_copy(source, target, off_sem.at[number])
            for number, (source, target) in enumerate(
                (
                    (start_hbm, start_ref),
                    (sends_hbm, sends_ref),
                    (agg_hbm, agg_ref),
                    (near_hbm, near_ref),
                    (diag_hbm, diag_ref),
                    (cols_hbm, cols_ref),
                )
            )
        ]
        cuts = [(16 * v, min(16, slots - 16 * v)) for v in range(gunits)]
        loads += [
            pltpu.make_async_copy(
                off_hbm.at[:, pl.ds(k, count)], off_v.at[:, pl.ds(k, count)], off_sem.at[len(loads) + v]
            )
            for v, (k, count) in enumerate(cuts)
        ]
        for number in LOAD_ORDER + list(range(len(LOAD_ORDER), len(loads))):
            loads[number].start()

        def clear(place):
            cleared = [recvw.at[:, place]]
            if place < len(WAYS):
                cleared += [recvu.at[:, place], recvg.at[place], recvt.at[place]]
            for ref in cleared:
                ref[...] = jnp.zeros(ref.shape, jnp.float32)

        for place, (x, y) in enumerate(CIRCLE):
            pl.when(jnp.logical_not(present(-x, -y)))(functools.partial(clear, place))

        def remote(source, target, sent, came, place):
            x, y = CIRCLE[place]
            return pltpu.make_async_remote_copy(
                src_ref=source, dst_ref=target, send_sem=sent, recv_sem=came,
                device_id={"slab": a + x, "sub": b + y}, device_id_type=MESH,
            )

        def w_copy(turn, place):
            return remote(
                sendw.at[turn], recvw.at[turn, place],
                sendw_sem.at[place], recvw_sem.at[lax.rem(turn, 2), place], place,
            )

        def u_copy(turn, way):
            return remote(
                sendu.at[turn], recvu.at[turn, way],
                sendu_sem.at[way], recvu_sem.at[lax.rem(turn, 2), way], way,
            )

        def g_copy(v, way):
            return remote(
                sendg.at[way, v], recvg.at[way, v], sendg_sem.at[way], recvg_sem.at[way], way
            )

        def g_whole(way):
            return remote(sendg.at[way], recvg.at[way], sendg_sem.at[way], recvg_sem.at[way], way)

        def t_copy(way):
            return remote(sendt.at[way // 2], recvt.at[way], sendt_sem.at[way], recvt_sem.at[way], way)

        def each_target(make, places, act):
            for place in places:
                x, y = CIRCLE[place]
                pl.when(present(x, y))(functools.partial(lambda place: act(make(place)), place))

        def each_source(make, places):
            for place in places:
                x, y = CIRCLE[place]
                pl.when(present(-x, -y))(functools.partial(lambda place: make(place).wait_recv(), place))

        def begin_copy(copy):
            copy.start()

        def settle(copy):
            copy.wait_send()

        ways = range(len(WAYS))
        far = range(len(WAYS), len(CIRCLE))
        left = lax.broadcasted_iota(jnp.int32, (8, LANES), 1) < half

        hist[...] = jnp.zeros_like(hist)
        loads[0].wait()
        loads[1].wait()
        hist[0, 0:3, :] = start_ref[...]
        for pair in range(2):
            sidx[pair] = jnp.broadcast_to(
                jnp.concatenate(
                    [sends_ref[2 * pair : 2 * pair + 1, :], sends_ref[2 * pair + 1 : 2 * pair + 2, :]],
                    axis=1,
                ),
                (8, LANES),
            )

        def listed(step):
            tables = [hist[step, :, tile(j)] for j in range(tiles)]
            picked = [pick(tables, sidx[pair], 0) for pair in range(2)]
            return jnp.concatenate([picked[0][0:4], picked[1][0:4]], axis=0)

        sendw[...] = jnp.zeros_like(sendw)
        sendu[...] = jnp.zeros_like(sendu)
        sendw[0] = listed(0)

        loads[4].wait()
        loads[5].wait()
        inverse = invert_rows([diag_ref[p : p + 1, :] for p in range(9)])
        for p in range(9):
            dinv[p : p + 1, :] = inverse[p]
        rest_m[...] = jnp.zeros_like(rest_m)
        for u, places in enumerate(units):
            if len(places) * places[0][2] < 8:
                cols_u[u] = jnp.zeros((8, LANES), jnp.int32)
            for at, k, count, j in places:
                cols_u[u, at : at + count, :] = cols_ref[k : k + count, tile(j)]
                if count < 8:
                    rest_m[planes - 1, j, 0:count, :] = cols_ref[k : k + count, tile(j)].astype(jnp.float32)

        def source(q, group, j):
            if 8 * (group + 1) > slots:
                return rest_m[q, j]
            u = group * tiles + j
            return cols_u[u].astype(jnp.float32) if q == planes - 1 else mats[u, q]

        def chosen(q, group, pair):
            if group >= groups:
                return jnp.zeros((8, LANES), jnp.float32)
            return pick([source(q, group, j) for j in range(tiles)], sidx[pair], 0)

        for v, (cut, length) in enumerate(cuts):
            loads[6 + v].wait()
            for u, places in enumerate(units):
                if not cut <= places[0][1] < cut + length:
                    continue
                if len(places) * places[0][2] < 8:
                    mats[u] = jnp.zeros(mats.shape[1:], jnp.float32)
                for at, k, count, j in places:
                    block = [off_v[p, k : k + count, tile(j)] for p in range(9)]
                    for r in range(3):
                        scale = [
                            jnp.broadcast_to(dinv[3 * r + q : 3 * r + q + 1, tile(j)], (count, LANES))
                            for q in range(3)
                        ]
                        for c in range(3):
                            entry = scale[0] * block[c] + scale[1] * block[3 + c] + scale[2] * block[6 + c]
                            mats[u, 3 * r + c, at : at + count, :] = entry
                            if count < 8:
                                rest_m[3 * r + c, j, 0:count, :] = entry
            for pair in (1, 0):
                for q in range(planes):
                    low = chosen(q, 2 * v, pair)
                    high = chosen(q, 2 * v + 1, pair)
                    for group, listing in ((2 * v, low), (2 * v + 1, high)):
                        if group < groups and q < planes - 1:
                            mine[pair, group, q] = listing
                        elif group < groups:
                            minecol[pair, group] = listing.astype(jnp.int32)
                    sendg[2 * pair, v, q] = jnp.where(left, low, pltpu.roll(high, half, 1))
                    sendg[2 * pair + 1, v, q] = jnp.where(left, pltpu.roll(low, half, 1), high)
                if v == 0 and pair == 1:
                    pl.semaphore_wait(barrier, greeters)
                    each_target(functools.partial(w_copy, 0), ORDER, begin_copy)
                each_target(functools.partial(g_copy, v), (2 * pair, 2 * pair + 1), begin_copy)

        def tentative():
            loads[2].wait()
            loads[3].wait()
            agg = agg_ref[...]
            member = (
                jnp.broadcast_to(agg, (sizes_of, rows)) == lax.broadcasted_iota(jnp.int32, (sizes_of, rows), 0)
            ).astype(jnp.float32)
            counts = jnp.sum(member, axis=1, keepdims=True)
            sizes = jnp.sum(member * counts, axis=0, keepdims=True)
            tent_ref[...] = near_ref[...] * lax.rsqrt(sizes)
            text[...] = jnp.zeros_like(text)
            for c in range(3):
                text[8 * c : 8 * c + modes, 0:rows] = tent_ref[modes * c : modes * (c + 1), :]
            for pair in range(2):
                for c in range(3):
                    sendt[pair, 8 * c : 8 * c + 8, :] = pick(
                        [text[8 * c : 8 * c + 8, tile(j)] for j in range(tiles)], sidx[pair], 0
                    )
            each_target(t_copy, ways, begin_copy)

        per = -(-len(units) // (BLOCKS - 1))

        def spread(row):
            return jnp.broadcast_to(row, (8, LANES))

        def unit_products(u, unused):
            index = cols_u[u]
            for m in range(modes):
                picked = [
                    pick(
                        [
                            spread(text[8 * c + m : 8 * c + m + 1, tile(i)])
                            for i in range(tiles + 2)
                        ],
                        index,
                        0,
                    )
                    for c in range(3)
                ]
                for r in range(3):
                    raw_ref[modes * r + m, u] = (
                        mats[u, 3 * r] * picked[0]
                        + mats[u, 3 * r + 1] * picked[1]
                        + mats[u, 3 * r + 2] * picked[2]
                    )
            return unused

        def contribute(tables, first, u):
            index = cols_u[u]
            picked = [pick(tables[c], index, first) for c in range(3)]
            return [sum(mats[u, 3 * r + c] * picked[c] for c in range(3)) for r in range(3)]

        def contribute_near(tables, first, way):
            total = [None] * 3
            for v in range(gunits):
                index = gcol[way, v]
                picked = [pick(tables[c], index, first) for c in range(3)]
                for r in range(3):
                    term = sum(recvg[way, v, 3 * r + c] * picked[c] for c in range(3))
                    total[r] = term if total[r] is None else total[r] + term
            return total

        def contribute_mine(tables, first):
            total = [[None] * 3 for pair in range(2)]
            for pair in range(2):
                for group in range(groups):
                    index = minecol[pair, group]
                    picked = [pick(tables[c], index, first) for c in range(3)]
                    for r in range(3):
                        term = sum(mine[pair, group, 3 * r + c] * picked[c] for c in range(3))
                        total[pair][r] = term if group == 0 else total[pair][r] + term
            return total

        def own_tables(step):
            return [[spread(hist[step, c : c + 1, tile(i)]) for i in range(tiles)] for c in range(3)]

        def by_tile(terms):
            whole = [[None] * tiles for r in range(3)]
            for r in range(3):
                for u, places in enumerate(units):
                    if len(places) == 1 and places[0][2] == 8:
                        j = places[0][3]
                        old = whole[r][j]
                        whole[r][j] = terms[u][r] if old is None else old + terms[u][r]
                for j in range(tiles):
                    old = whole[r][j]
                    whole[r][j] = 0.0 if old is None else jnp.sum(old, axis=0, keepdims=True)
                for u, places in enumerate(units):
                    if not (len(places) == 1 and places[0][2] == 8):
                        for at, k, count, j in places:
                            whole[r][j] = whole[r][j] + jnp.sum(
                                terms[u][r][at : at + count], axis=0, keepdims=True
                            )
            return whole

        def own_part(step):
            tables = own_tables(step)
            inner = by_tile([contribute(tables, 0, u) for u in range(len(units))])
            for r in range(3):
                for j in range(tiles):
                    hist[step + 1, r : r + 1, tile(j)] = hist[step, r : r + 1, tile(j)] + inner[r][j]

        def ghost_part(step, tables):
            outer = by_tile([contribute(tables, tiles, u) for u in range(len(units))])
            for r in range(3):
                for j in range(tiles):
                    hist[step + 1, r : r + 1, tile(j)] = hist[step + 1, r : r + 1, tile(j)] + outer[r][j]

        def halves(first, second, pair):
            both = jnp.where(left, first, second)
            return [both[4 * pair + c : 4 * pair + c + 1] for c in range(3)]

        def iterate(turn, last):
            step = DEPTH * turn
            inner = contribute_mine(own_tables(step), 0)
            for pair in range(2):
                for r in range(3):
                    at = pl.ds(4 * pair + r, 1)
                    sendu[turn, at, :] = sendw[turn, at, :] + jnp.sum(inner[pair][r], axis=0, keepdims=True)
            each_target(functools.partial(u_copy, turn), ways, begin_copy)
            own_part(step)
            pl.when(turn == 0)(tentative)

            @pl.when(turn == 1)
            def _():
                each_source(t_copy, ways)
                for pair in range(2):
                    for c in range(3):
                        text[8 * c : 8 * c + 8, tile(tiles + pair)] = jnp.where(
                            left,
                            recvt[2 * pair, 8 * c : 8 * c + 8, :],
                            recvt[2 * pair + 1, 8 * c : 8 * c + 8, :],
                        )

            lax.fori_loop(
                jnp.clip((turn - 1) * per, 0, len(units)), jnp.clip(turn * per, 0, len(units)), unit_products, 0
            )
            each_target(functools.partial(w_copy, turn), ORDER, settle)
            each_target(functools.partial(u_copy, turn), ways, settle)
            each_source(functools.partial(w_copy, turn), ways)
            merged = [halves(recvw[turn, 2 * pair], recvw[turn, 2 * pair + 1], pair) for pair in range(2)]
            ghost_part(step, [[spread(merged[pair][c]) for pair in range(2)] for c in range(3)])
            if last:
                own_part(step + 1)
                stat[0, 1:2, :] = squares(step + 1)
            else:
                kept = listed(step + 1)
                inner = contribute_mine(own_tables(step + 1), 0)

            @pl.when(turn == 0)
            def _():
                each_source(g_whole, ways)
                for way in ways:
                    for v in range(gunits):
                        gcol[way, v] = recvg[way, v, planes - 1].astype(jnp.int32)

            each_source(functools.partial(w_copy, turn), far)

            def packed(way, other):
                x, y = (WAYS[way][axis] + WAYS[other][axis] for axis in range(2))
                return sendw[turn] if (x, y) == (0, 0) else recvw[turn, CIRCLE.index((x, y))]

            total = []
            for way in ways:
                rows_of = [
                    halves(packed(way, 2 * pair), packed(way, 2 * pair + 1), pair) for pair in range(2)
                ]
                total.append(
                    contribute_near(
                        [[spread(rows_of[pair][c]) for pair in range(2)] for c in range(3)], tiles, way
                    )
                )
            each_source(functools.partial(u_copy, turn), ways)
            base = [halves(recvu[turn, 2 * pair], recvu[turn, 2 * pair + 1], pair) for pair in range(2)]
            later = [[], [], []]
            for r in range(3):
                for pair in range(2):
                    first, second = total[2 * pair][r], total[2 * pair + 1][r]
                    both = jnp.where(left, first, second) + pltpu.roll(
                        jnp.where(left, second, first), half, 1
                    )
                    later[r].append(spread(base[pair][r] + jnp.sum(both, axis=0, keepdims=True)))
            if last:
                ghost_part(step + 1, later)
                return
            outer = contribute_mine(later, tiles)
            for pair in range(2):
                for r in range(3):
                    row = 4 * pair + r
                    sendw[turn + 1, row : row + 1, :] = kept[row : row + 1] + jnp.sum(
                        inner[pair][r] + outer[pair][r], axis=0, keepdims=True
                    )
            each_target(functools.partial(w_copy, turn + 1), ORDER, begin_copy)
            own_part(step + 1)
            ghost_part(step + 1, later)

        def squares(step):
            return jnp.sum(
                sum(hist[step, :, tile(j)] * hist[step, :, tile(j)] for j in range(tiles)),
                axis=0, keepdims=True,
            )

        def advance(turn, unused):
            iterate(turn, False)
            return unused

        lax.fori_loop(0, BLOCKS - 1, advance, 0)
        iterate(BLOCKS - 1, True)

        stat[0, 0:1, :] = squares(ITERS)
        me = a * n_sub + b

        def begin(step, unused):
            target = lax.rem(me + jnp.where(2 * a < n_slab, devices - step, step), devices)
            pltpu.make_async_remote_copy(
                src_ref=stat.at[0], dst_ref=stats.at[me], send_sem=ss_sem, recv_sem=rs_sem,
                device_id={"slab": lax.div(target, n_sub), "sub": lax.rem(target, n_sub)},
                device_id_type=MESH,
            ).start()
            return unused

        lax.fori_loop(1, devices, begin, 0, unroll=devices <= 64)
        stats[me] = stat[0]
        each_target(g_whole, ways, settle)
        each_target(t_copy, ways, settle)

    dma = pltpu.SemaphoreType.DMA
    ways = len(WAYS)
    pl.run_scoped(
        power,
        dma((6 + sendg.shape[1],)),
        dma((len(CIRCLE),)),
        dma((2, len(CIRCLE))),
        dma((ways,)),
        dma((2, ways)),
        dma((ways,)),
        dma((ways,)),
        dma((ways,)),
        dma((ways,)),
    )
    others = stats.at[pl.ds(0, devices - 1)]
    everything = pltpu.make_async_remote_copy(
        src_ref=others, dst_ref=others, send_sem=ss_sem, recv_sem=rs_sem,
        device_id={"slab": n_slab - 1 - a, "sub": n_sub - 1 - b}, device_id_type=MESH,
    )
    everything.wait_recv()
    whole = jnp.sum(stats[...], axis=0)
    total = jnp.sum(whole, axis=1, keepdims=True)
    latest = total[0:1]
    previous = total[1:2]
    rho_ref[...] = jnp.sqrt(latest / (previous + 1e-05))

    everything.wait_send()


def body(n_slab, n_sub, near_null, aggregates, diag_block, off_blocks, columns, sends, start_vector):
    slots, nine, rows = off_blocks.shape
    wide = rows + 2 * LANES
    count = len(unit_places(slots, rows // LANES))
    gunits = -(-slots // 16)
    f32 = jnp.float32
    vmem = pl.BlockSpec(memory_space=pltpu.VMEM)
    dma = pltpu.SemaphoreType.DMA
    raw, tentative, rho = pl.pallas_call(
        functools.partial(kernel, n_slab, n_sub),
        out_shape=(
            pltpu.VMEM((near_null.shape[0], count, 8, LANES), f32),
            pltpu.VMEM(near_null.shape, f32),
            jax.ShapeDtypeStruct((1, 1), f32),
        ),
        in_specs=[pl.BlockSpec(memory_space=pltpu.HBM)] * 7,
        out_specs=(vmem, vmem, vmem),
        scratch_shapes=[
            pltpu.VMEM(near_null.shape, f32),
            pltpu.VMEM((1, rows), jnp.int32),
            pltpu.VMEM(diag_block.shape, f32),
            pltpu.VMEM(columns.shape, jnp.int32),
            pltpu.VMEM(sends.shape, jnp.int32),
            pltpu.VMEM(start_vector.shape, f32),
            pltpu.VMEM((nine, slots, rows), f32),
            pltpu.VMEM((count, 8, LANES), jnp.int32),
            pltpu.VMEM((count, nine, 8, LANES), f32),
            pltpu.VMEM((nine + 1, rows // LANES, 8, LANES), f32),
            pltpu.VMEM((16, rows), f32),
            pltpu.VMEM((24, wide), f32),
            pltpu.VMEM((ITERS + 1, 8, rows), f32),
            pltpu.VMEM((2, 8, LANES), jnp.int32),
            pltpu.VMEM((BLOCKS, 8, LANES), f32),
            pltpu.VMEM((BLOCKS, len(CIRCLE), 8, LANES), f32),
            pltpu.VMEM((BLOCKS, 8, LANES), f32),
            pltpu.VMEM((BLOCKS, len(WAYS), 8, LANES), f32),
            pltpu.VMEM((2, -(-slots // 8), nine, 8, LANES), f32),
            pltpu.VMEM((2, -(-slots // 8), 8, LANES), jnp.int32),
            pltpu.VMEM((len(WAYS), gunits, nine + 1, 8, LANES), f32),
            pltpu.VMEM((len(WAYS), gunits, nine + 1, 8, LANES), f32),
            pltpu.VMEM((len(WAYS), gunits, 8, LANES), jnp.int32),
            pltpu.VMEM((2, 24, LANES), f32),
            pltpu.VMEM((4, 24, LANES), f32),
            pltpu.VMEM((1, 2, LANES), f32),
            pltpu.VMEM((n_slab * n_sub, 2, LANES), f32),
            dma,
            dma,
        ],
        compiler_params=pltpu.CompilerParams(collective_id=0, has_side_effects=True, vmem_limit_bytes=16777216),
        name="smooth",
    )(
        *[
            pltpu.with_memory_space_constraint(x, pltpu.HBM)
            for x in (
                near_null, aggregates.reshape(1, rows), diag_block, off_blocks.transpose(1, 0, 2),
                columns, sends, start_vector,
            )
        ]
    )
    prolong_off, prolong_self, rho = pl.pallas_call(
        scale_kernel,
        out_shape=(
            jax.ShapeDtypeStruct((near_null.shape[0], slots, rows), jnp.bfloat16),
            jax.ShapeDtypeStruct(near_null.shape, jnp.bfloat16),
            jax.ShapeDtypeStruct((1, 1), f32),
        ),
        in_specs=[vmem, vmem, vmem],
        out_specs=(vmem, vmem, vmem),
        compiler_params=pltpu.CompilerParams(vmem_limit_bytes=16777216),
        name="scale",
    )(raw, tentative, rho)
    return (prolong_off.transpose(1, 0, 2), prolong_self, rho.reshape(()))


def solution(mesh):
    placed = (
        P(None, ("slab", "sub")),
        P(("slab", "sub")),
        P(None, ("slab", "sub")),
        P(None, None, ("slab", "sub")),
        P(None, ("slab", "sub")),
        P(None, ("slab", "sub")),
        P(None, ("slab", "sub")),
    )
    return jax.shard_map(
        functools.partial(body, mesh.shape["slab"], mesh.shape["sub"]),
        mesh=mesh,
        in_specs=placed,
        out_specs=(P(None, None, ("slab", "sub")), P(None, ("slab", "sub")), P()),
        check_vma=False,
    )
```

```python
import functools

import jax
import jax.numpy as jnp
from jax import lax
from jax.experimental import pallas as pl
from jax.experimental.pallas import tpu as pltpu
from jax.sharding import PartitionSpec as P

ITERS = 8
OMEGA = 4.0 / 3.0
LANES = 128
MESH = pl.DeviceIdType.MESH
LOAD_ORDER = [0, 1, 4, 5, 2, 3]
DEPTH = 2
BLOCKS = ITERS // DEPTH
WAYS = [(0, 1), (0, -1), (1, 0), (-1, 0)]
FAR = [(-1, -1), (-1, 1), (1, -1), (1, 1), (-2, 0), (2, 0), (0, -2), (0, 2)]
CIRCLE = WAYS + FAR
ORDER = list(range(len(WAYS), len(CIRCLE))) + list(range(len(WAYS)))


def lane_gather(table, lanes):
    return jnp.take_along_axis(table, lanes, axis=1, mode="promise_in_bounds")


def tile(number):
    return pl.ds(number * LANES, LANES)


def pick(tables, index, first):
    high = index >> 7
    low = index & (LANES - 1)
    out = jnp.zeros(index.shape, jnp.float32)
    for step, table in enumerate(tables):
        out = jnp.where(high == first + step, lane_gather(table, low), out)
    return out


def invert_rows(entries):
    cofactor = [
        entries[4] * entries[8] - entries[5] * entries[7],
        entries[5] * entries[6] - entries[3] * entries[8],
        entries[3] * entries[7] - entries[4] * entries[6],
        entries[2] * entries[7] - entries[1] * entries[8],
        entries[0] * entries[8] - entries[2] * entries[6],
        entries[1] * entries[6] - entries[0] * entries[7],
        entries[1] * entries[5] - entries[2] * entries[4],
        entries[2] * entries[3] - entries[0] * entries[5],
        entries[0] * entries[4] - entries[1] * entries[3],
    ]
    determinant = entries[0] * cofactor[0] + entries[1] * cofactor[1] + entries[2] * cofactor[2]
    return [
        cofactor[column * 3 + row] / determinant for row in range(3) for column in range(3)
    ]


def unit_places(slots, tiles):
    units = []
    for k in range(0, slots - 7, 8):
        for j in range(tiles):
            units.append([(0, k, 8, j)])
    rest = slots % 8
    if rest:
        share = 8 // rest
        for j in range(0, tiles, share):
            units.append(
                [
                    (rest * i, slots - rest, rest, j + i)
                    for i in range(min(share, tiles - j))
                ]
            )
    return units


def scale_kernel(raw_ref, tent_ref, rho_ref, off_ref, self_ref, out_rho_ref):
    slots, rows = off_ref.shape[1:]
    out_rho_ref[...] = rho_ref[0:1, 0:1]
    inverse = OMEGA / rho_ref[...]
    factor = -inverse
    places = unit_places(slots, rows // LANES)
    for j in range(rows // LANES):
        for entry in range(off_ref.shape[0]):
            parts = [
                (raw_ref[entry, u] * factor)[at : at + count]
                for u in range(len(places))
                for at, k, count, tile_number in places[u]
                if tile_number == j
            ]
            off_ref[entry, :, tile(j)] = jnp.concatenate(parts, axis=0).astype(off_ref.dtype)
    self_ref[...] = ((1.0 - inverse[0:1, 0:1]) * tent_ref[...]).astype(self_ref.dtype)


def kernel(
    n_slab, n_sub,
    near_hbm, agg_hbm, diag_hbm, off_hbm, cols_hbm, sends_hbm, start_hbm,
    raw_ref, tent_ref, rho_ref,
    near_ref, agg_ref, diag_ref, cols_ref, sends_ref, start_ref, off_v, cols_u, mats, rest_m, dinv, text, hist, sidx,
    sendw, recvw, sendu, recvu, mine, minecol, sendg, recvg, gcol, sendt, recvt, stat, stats,
    ss_sem, rs_sem,
):
    a = lax.axis_index("slab")
    b = lax.axis_index("sub")
    devices = n_slab * n_sub

    def power(
        off_sem, sendw_sem, recvw_sem, sendu_sem, recvu_sem, sendg_sem, recvg_sem, sendt_sem, recvt_sem
    ):
        slots, rows = cols_ref.shape
        half = sends_ref.shape[1]
        tiles = rows // LANES
        units = unit_places(slots, tiles)
        groups = -(-slots // 8)
        gunits, planes = sendg.shape[1:3]
        modes = near_ref.shape[0] // 3
        sizes_of = rows // 8
        barrier = pltpu.get_barrier_semaphore()
        def present(x, y):
            return (a + x >= 0) & (a + x < n_slab) & (b + y >= 0) & (b + y < n_sub)

        def greet(x, y):
            pl.semaphore_signal(
                barrier, inc=1, device_id={"slab": a + x, "sub": b + y}, device_id_type=MESH
            )

        def greet_any(step, unused):
            target = lax.rem(a * n_sub + b + step, n_slab * n_sub)
            greet(lax.div(target, n_sub) - a, lax.rem(target, n_sub) - b)
            return unused

        near = n_slab - 1 + n_sub - 1 <= ITERS + 2
        if near:
            for x, y in CIRCLE:
                pl.when(present(x, y))(functools.partial(greet, x, y))
            greeters = sum(present(x, y).astype(jnp.int32) for x, y in CIRCLE)
        else:
            lax.fori_loop(1, n_slab * n_sub, greet_any, 0)
            greeters = n_slab * n_sub - 1

        loads = [
            pltpu.make_async_copy(source, target, off_sem.at[number])
            for number, (source, target) in enumerate(
                (
                    (start_hbm, start_ref),
                    (sends_hbm, sends_ref),
                    (agg_hbm, agg_ref),
                    (near_hbm, near_ref),
                    (diag_hbm, diag_ref),
                    (cols_hbm, cols_ref),
                )
            )
        ]
        deep = [min(8, -(-(slots - 16 * v) // 2)) for v in range(gunits)]
        cuts = [(16 * v, min(16, slots - 16 * v)) for v in range(gunits)]
        loads += [
            pltpu.make_async_copy(
                off_hbm.at[:, pl.ds(k, count)], off_v.at[:, pl.ds(k, count)], off_sem.at[len(loads) + v]
            )
            for v, (k, count) in enumerate(cuts)
        ]
        for number in LOAD_ORDER + list(range(len(LOAD_ORDER), len(loads))):
            loads[number].start()

        for way in range(len(WAYS)):
            for v in range(gunits):
                if deep[v] < 8:
                    recvg[way, v, :, deep[v] : 8, :] = jnp.zeros((planes, 8 - deep[v], LANES), jnp.float32)

        def clear(place):
            cleared = [recvw.at[:, place]]
            if place < len(WAYS):
                cleared += [recvu.at[:, place], recvg.at[place], recvt.at[place]]
            for ref in cleared:
                ref[...] = jnp.zeros(ref.shape, jnp.float32)

        for place, (x, y) in enumerate(CIRCLE):
            pl.when(jnp.logical_not(present(-x, -y)))(functools.partial(clear, place))

        def remote(source, target, sent, came, place):
            x, y = CIRCLE[place]
            return pltpu.make_async_remote_copy(
                src_ref=source, dst_ref=target, send_sem=sent, recv_sem=came,
                device_id={"slab": a + x, "sub": b + y}, device_id_type=MESH,
            )

        def w_copy(turn, place):
            return remote(
                sendw.at[turn], recvw.at[turn, place],
                sendw_sem.at[place], recvw_sem.at[lax.rem(turn, 2), place], place,
            )

        def u_copy(turn, way):
            return remote(
                sendu.at[turn], recvu.at[turn, way],
                sendu_sem.at[way], recvu_sem.at[lax.rem(turn, 2), way], way,
            )

        def g_copy(v, way):
            part = pl.ds(0, deep[v])
            return remote(
                sendg.at[way, v, :, part], recvg.at[way, v, :, part],
                sendg_sem.at[way, v], recvg_sem.at[way, v], way,
            )

        def t_copy(way):
            return remote(sendt.at[way // 2], recvt.at[way], sendt_sem.at[way], recvt_sem.at[way], way)

        def each_target(make, places, act):
            for place in places:
                x, y = CIRCLE[place]
                pl.when(present(x, y))(functools.partial(lambda place: act(make(place)), place))

        def each_source(make, places):
            for place in places:
                x, y = CIRCLE[place]
                pl.when(present(-x, -y))(functools.partial(lambda place: make(place).wait_recv(), place))

        def begin_copy(copy):
            copy.start()

        def settle(copy):
            copy.wait_send()

        ways = range(len(WAYS))
        far = range(len(WAYS), len(CIRCLE))
        left = lax.broadcasted_iota(jnp.int32, (8, LANES), 1) < half

        hist[...] = jnp.zeros_like(hist)
        loads[0].wait()
        loads[1].wait()
        hist[0, 0:3, :] = start_ref[...]
        for pair in range(2):
            sidx[pair] = jnp.broadcast_to(
                jnp.concatenate(
                    [sends_ref[2 * pair : 2 * pair + 1, :], sends_ref[2 * pair + 1 : 2 * pair + 2, :]],
                    axis=1,
                ),
                (8, LANES),
            )

        def listed(step):
            tables = [hist[step, :, tile(j)] for j in range(tiles)]
            picked = [pick(tables, sidx[pair], 0) for pair in range(2)]
            return jnp.concatenate([picked[0][0:4], picked[1][0:4]], axis=0)

        sendw[...] = jnp.zeros_like(sendw)
        sendu[...] = jnp.zeros_like(sendu)
        sendw[0] = listed(0)

        loads[4].wait()
        loads[5].wait()
        inverse = invert_rows([diag_ref[p : p + 1, :] for p in range(9)])
        for p in range(9):
            dinv[p : p + 1, :] = inverse[p]
        rest_m[...] = jnp.zeros_like(rest_m)
        for u, places in enumerate(units):
            if len(places) * places[0][2] < 8:
                cols_u[u] = jnp.zeros((8, LANES), jnp.int32)
            for at, k, count, j in places:
                cols_u[u, at : at + count, :] = cols_ref[k : k + count, tile(j)]
                if count < 8:
                    rest_m[planes - 1, j, 0:count, :] = cols_ref[k : k + count, tile(j)].astype(jnp.float32)

        def source(q, group, j):
            if 8 * (group + 1) > slots:
                return rest_m[q, j]
            u = group * tiles + j
            return cols_u[u].astype(jnp.float32) if q == planes - 1 else mats[u, q]

        def chosen(q, group, pair):
            if group >= groups:
                return jnp.zeros((8, LANES), jnp.float32)
            return pick([source(q, group, j) for j in range(tiles)], sidx[pair], 0)

        for v, (cut, length) in enumerate(cuts):
            loads[6 + v].wait()
            for u, places in enumerate(units):
                if not cut <= places[0][1] < cut + length:
                    continue
                if len(places) * places[0][2] < 8:
                    mats[u] = jnp.zeros(mats.shape[1:], jnp.float32)
                for at, k, count, j in places:
                    block = [off_v[p, k : k + count, tile(j)] for p in range(9)]
                    for r in range(3):
                        scale = [
                            jnp.broadcast_to(dinv[3 * r + q : 3 * r + q + 1, tile(j)], (count, LANES))
                            for q in range(3)
                        ]
                        for c in range(3):
                            entry = scale[0] * block[c] + scale[1] * block[3 + c] + scale[2] * block[6 + c]
                            mats[u, 3 * r + c, at : at + count, :] = entry
                            if count < 8:
                                rest_m[3 * r + c, j, 0:count, :] = entry
        def pack_rows(v, pair):
            count = deep[v]
            for q in range(planes):
                low = chosen(q, 2 * v, pair)
                high = chosen(q, 2 * v + 1, pair)
                for group, listing in ((2 * v, low), (2 * v + 1, high)):
                    if group < groups and q < planes - 1:
                        mine[pair, group, q] = listing
                    elif group < groups:
                        minecol[pair, group] = listing.astype(jnp.int32)
                if count < 8:
                    high = jnp.concatenate([low[count:8], high[0:count]], axis=0)
                sendg[2 * pair, v, q] = jnp.where(left, low, pltpu.roll(high, half, 1))
                sendg[2 * pair + 1, v, q] = jnp.where(left, pltpu.roll(low, half, 1), high)

        for number, (v, pair) in enumerate([(v, pair) for v in range(gunits) for pair in (0, 1)]):
            pack_rows(v, pair)
            if number == 0:
                pl.semaphore_wait(barrier, greeters)
                each_target(functools.partial(w_copy, 0), ORDER, begin_copy)
            each_target(functools.partial(g_copy, v), (2 * pair, 2 * pair + 1), begin_copy)

        def tentative():
            loads[2].wait()
            loads[3].wait()
            agg = agg_ref[...]
            member = (
                jnp.broadcast_to(agg, (sizes_of, rows)) == lax.broadcasted_iota(jnp.int32, (sizes_of, rows), 0)
            ).astype(jnp.float32)
            counts = jnp.sum(member, axis=1, keepdims=True)
            sizes = jnp.sum(member * counts, axis=0, keepdims=True)
            tent_ref[...] = near_ref[...] * lax.rsqrt(sizes)
            text[...] = jnp.zeros_like(text)
            for c in range(3):
                text[8 * c : 8 * c + modes, 0:rows] = tent_ref[modes * c : modes * (c + 1), :]
            for pair in range(2):
                for c in range(3):
                    sendt[pair, 8 * c : 8 * c + 8, :] = pick(
                        [text[8 * c : 8 * c + 8, tile(j)] for j in range(tiles)], sidx[pair], 0
                    )
            each_target(t_copy, ways, begin_copy)

        per = -(-len(units) // (BLOCKS - 1))

        def spread(row):
            return jnp.broadcast_to(row, (8, LANES))

        def unit_products(u, unused):
            index = cols_u[u]
            for m in range(modes):
                picked = [
                    pick(
                        [
                            spread(text[8 * c + m : 8 * c + m + 1, tile(i)])
                            for i in range(tiles + 2)
                        ],
                        index,
                        0,
                    )
                    for c in range(3)
                ]
                for r in range(3):
                    raw_ref[modes * r + m, u] = (
                        mats[u, 3 * r] * picked[0]
                        + mats[u, 3 * r + 1] * picked[1]
                        + mats[u, 3 * r + 2] * picked[2]
                    )
            return unused

        def contribute(tables, first, u):
            index = cols_u[u]
            picked = [pick(tables[c], index, first) for c in range(3)]
            return [sum(mats[u, 3 * r + c] * picked[c] for c in range(3)) for r in range(3)]

        def contribute_near(tables, first, way):
            total = [None] * 3
            for v in range(gunits):
                index = gcol[way, v]
                picked = [pick(tables[c], index, first) for c in range(3)]
                for r in range(3):
                    term = sum(recvg[way, v, 3 * r + c] * picked[c] for c in range(3))
                    total[r] = term if total[r] is None else total[r] + term
            return total

        def contribute_mine(tables, first):
            total = [[None] * 3 for pair in range(2)]
            for pair in range(2):
                for group in range(groups):
                    index = minecol[pair, group]
                    picked = [pick(tables[c], index, first) for c in range(3)]
                    for r in range(3):
                        term = sum(mine[pair, group, 3 * r + c] * picked[c] for c in range(3))
                        total[pair][r] = term if group == 0 else total[pair][r] + term
            return total

        def own_tables(step):
            return [[spread(hist[step, c : c + 1, tile(i)]) for i in range(tiles)] for c in range(3)]

        def by_tile(terms):
            whole = [[None] * tiles for r in range(3)]
            for r in range(3):
                for u, places in enumerate(units):
                    if len(places) == 1 and places[0][2] == 8:
                        j = places[0][3]
                        old = whole[r][j]
                        whole[r][j] = terms[u][r] if old is None else old + terms[u][r]
                for j in range(tiles):
                    old = whole[r][j]
                    whole[r][j] = 0.0 if old is None else jnp.sum(old, axis=0, keepdims=True)
                for u, places in enumerate(units):
                    if not (len(places) == 1 and places[0][2] == 8):
                        for at, k, count, j in places:
                            whole[r][j] = whole[r][j] + jnp.sum(
                                terms[u][r][at : at + count], axis=0, keepdims=True
                            )
            return whole

        def own_part(step):
            tables = own_tables(step)
            inner = by_tile([contribute(tables, 0, u) for u in range(len(units))])
            for r in range(3):
                for j in range(tiles):
                    hist[step + 1, r : r + 1, tile(j)] = hist[step, r : r + 1, tile(j)] + inner[r][j]

        def ghost_part(step, tables):
            outer = by_tile([contribute(tables, tiles, u) for u in range(len(units))])
            for r in range(3):
                for j in range(tiles):
                    hist[step + 1, r : r + 1, tile(j)] = hist[step + 1, r : r + 1, tile(j)] + outer[r][j]

        def halves(first, second, pair):
            both = jnp.where(left, first, second)
            return [both[4 * pair + c : 4 * pair + c + 1] for c in range(3)]

        def iterate(turn, last):
            step = DEPTH * turn
            inner = contribute_mine(own_tables(step), 0)
            for pair in range(2):
                for r in range(3):
                    at = pl.ds(4 * pair + r, 1)
                    sendu[turn, at, :] = sendw[turn, at, :] + jnp.sum(inner[pair][r], axis=0, keepdims=True)
            each_target(functools.partial(u_copy, turn), ways, begin_copy)
            own_part(step)
            pl.when(turn == 0)(tentative)

            @pl.when(turn == 1)
            def _():
                each_source(t_copy, ways)
                for pair in range(2):
                    for c in range(3):
                        text[8 * c : 8 * c + 8, tile(tiles + pair)] = jnp.where(
                            left,
                            recvt[2 * pair, 8 * c : 8 * c + 8, :],
                            recvt[2 * pair + 1, 8 * c : 8 * c + 8, :],
                        )

            lax.fori_loop(
                jnp.clip((turn - 1) * per, 0, len(units)), jnp.clip(turn * per, 0, len(units)), unit_products, 0
            )
            each_target(functools.partial(w_copy, turn), ORDER, settle)
            each_target(functools.partial(u_copy, turn), ways, settle)
            each_source(functools.partial(w_copy, turn), ways)
            merged = [halves(recvw[turn, 2 * pair], recvw[turn, 2 * pair + 1], pair) for pair in range(2)]
            ghost_part(step, [[spread(merged[pair][c]) for pair in range(2)] for c in range(3)])
            if last:
                own_part(step + 1)
                stat[0, 1:2, :] = squares(step + 1)
            else:
                kept = listed(step + 1)
                inner = contribute_mine(own_tables(step + 1), 0)

            @pl.when(turn == 0)
            def _():
                for v in range(gunits):
                    each_source(functools.partial(g_copy, v), ways)
                for way in ways:
                    for v in range(gunits):
                        gcol[way, v] = recvg[way, v, planes - 1].astype(jnp.int32)

            each_source(functools.partial(w_copy, turn), far)

            def packed(way, other):
                x, y = (WAYS[way][axis] + WAYS[other][axis] for axis in range(2))
                return sendw[turn] if (x, y) == (0, 0) else recvw[turn, CIRCLE.index((x, y))]

            total = []
            for way in ways:
                rows_of = [
                    halves(packed(way, 2 * pair), packed(way, 2 * pair + 1), pair) for pair in range(2)
                ]
                total.append(
                    contribute_near(
                        [[spread(rows_of[pair][c]) for pair in range(2)] for c in range(3)], tiles, way
                    )
                )
            each_source(functools.partial(u_copy, turn), ways)
            base = [halves(recvu[turn, 2 * pair], recvu[turn, 2 * pair + 1], pair) for pair in range(2)]
            later = [[], [], []]
            for r in range(3):
                for pair in range(2):
                    first, second = total[2 * pair][r], total[2 * pair + 1][r]
                    both = jnp.where(left, first, second) + pltpu.roll(
                        jnp.where(left, second, first), half, 1
                    )
                    later[r].append(spread(base[pair][r] + jnp.sum(both, axis=0, keepdims=True)))
            if last:
                ghost_part(step + 1, later)
                return
            outer = contribute_mine(later, tiles)
            for pair in range(2):
                for r in range(3):
                    row = 4 * pair + r
                    sendw[turn + 1, row : row + 1, :] = kept[row : row + 1] + jnp.sum(
                        inner[pair][r] + outer[pair][r], axis=0, keepdims=True
                    )
            each_target(functools.partial(w_copy, turn + 1), ORDER, begin_copy)
            own_part(step + 1)
            ghost_part(step + 1, later)

        def squares(step):
            return jnp.sum(
                sum(hist[step, :, tile(j)] * hist[step, :, tile(j)] for j in range(tiles)),
                axis=0, keepdims=True,
            )

        def advance(turn, unused):
            iterate(turn, False)
            return unused

        lax.fori_loop(0, BLOCKS - 1, advance, 0)
        iterate(BLOCKS - 1, True)

        stat[0, 0:1, :] = squares(ITERS)
        me = a * n_sub + b

        def begin(step, unused):
            target = lax.rem(me + jnp.where(2 * a < n_slab, devices - step, step), devices)
            pltpu.make_async_remote_copy(
                src_ref=stat.at[0], dst_ref=stats.at[me], send_sem=ss_sem, recv_sem=rs_sem,
                device_id={"slab": lax.div(target, n_sub), "sub": lax.rem(target, n_sub)},
                device_id_type=MESH,
            ).start()
            return unused

        lax.fori_loop(1, devices, begin, 0, unroll=devices <= 64)
        stats[me] = stat[0]
        for v in range(gunits):
            each_target(functools.partial(g_copy, v), ways, settle)
        each_target(t_copy, ways, settle)

    dma = pltpu.SemaphoreType.DMA
    ways = len(WAYS)
    pl.run_scoped(
        power,
        dma((6 + sendg.shape[1],)),
        dma((len(CIRCLE),)),
        dma((2, len(CIRCLE))),
        dma((ways,)),
        dma((2, ways)),
        dma((ways, sendg.shape[1])),
        dma((ways, sendg.shape[1])),
        dma((ways,)),
        dma((ways,)),
    )
    others = stats.at[pl.ds(0, devices - 1)]
    everything = pltpu.make_async_remote_copy(
        src_ref=others, dst_ref=others, send_sem=ss_sem, recv_sem=rs_sem,
        device_id={"slab": n_slab - 1 - a, "sub": n_sub - 1 - b}, device_id_type=MESH,
    )
    everything.wait_recv()
    whole = jnp.sum(stats[...], axis=0)
    total = jnp.sum(whole, axis=1, keepdims=True)
    latest = total[0:1]
    previous = total[1:2]
    rho_ref[...] = jnp.broadcast_to(jnp.sqrt(latest / (previous + 1e-05)), rho_ref.shape)

    everything.wait_send()


def body(n_slab, n_sub, near_null, aggregates, diag_block, off_blocks, columns, sends, start_vector):
    slots, nine, rows = off_blocks.shape
    wide = rows + 2 * LANES
    count = len(unit_places(slots, rows // LANES))
    gunits = -(-slots // 16)
    f32 = jnp.float32
    vmem = pl.BlockSpec(memory_space=pltpu.VMEM)
    dma = pltpu.SemaphoreType.DMA
    raw, tentative, rho = pl.pallas_call(
        functools.partial(kernel, n_slab, n_sub),
        out_shape=(
            pltpu.VMEM((near_null.shape[0], count, 8, LANES), f32),
            pltpu.VMEM(near_null.shape, f32),
            pltpu.VMEM((8, LANES), f32),
        ),
        in_specs=[pl.BlockSpec(memory_space=pltpu.HBM)] * 7,
        out_specs=(vmem, vmem, vmem),
        scratch_shapes=[
            pltpu.VMEM(near_null.shape, f32),
            pltpu.VMEM((1, rows), jnp.int32),
            pltpu.VMEM(diag_block.shape, f32),
            pltpu.VMEM(columns.shape, jnp.int32),
            pltpu.VMEM(sends.shape, jnp.int32),
            pltpu.VMEM(start_vector.shape, f32),
            pltpu.VMEM((nine, slots, rows), f32),
            pltpu.VMEM((count, 8, LANES), jnp.int32),
            pltpu.VMEM((count, nine, 8, LANES), f32),
            pltpu.VMEM((nine + 1, rows // LANES, 8, LANES), f32),
            pltpu.VMEM((16, rows), f32),
            pltpu.VMEM((24, wide), f32),
            pltpu.VMEM((ITERS + 1, 8, rows), f32),
            pltpu.VMEM((2, 8, LANES), jnp.int32),
            pltpu.VMEM((BLOCKS, 8, LANES), f32),
            pltpu.VMEM((BLOCKS, len(CIRCLE), 8, LANES), f32),
            pltpu.VMEM((BLOCKS, 8, LANES), f32),
            pltpu.VMEM((BLOCKS, len(WAYS), 8, LANES), f32),
            pltpu.VMEM((2, -(-slots // 8), nine, 8, LANES), f32),
            pltpu.VMEM((2, -(-slots // 8), 8, LANES), jnp.int32),
            pltpu.VMEM((len(WAYS), gunits, nine + 1, 8, LANES), f32),
            pltpu.VMEM((len(WAYS), gunits, nine + 1, 8, LANES), f32),
            pltpu.VMEM((len(WAYS), gunits, 8, LANES), jnp.int32),
            pltpu.VMEM((2, 24, LANES), f32),
            pltpu.VMEM((4, 24, LANES), f32),
            pltpu.VMEM((1, 2, LANES), f32),
            pltpu.VMEM((n_slab * n_sub, 2, LANES), f32),
            dma,
            dma,
        ],
        compiler_params=pltpu.CompilerParams(collective_id=0, has_side_effects=True, vmem_limit_bytes=16777216),
        name="smooth",
    )(
        *[
            pltpu.with_memory_space_constraint(x, pltpu.HBM)
            for x in (
                near_null, aggregates.reshape(1, rows), diag_block, off_blocks.transpose(1, 0, 2),
                columns, sends, start_vector,
            )
        ]
    )
    prolong_off, prolong_self, rho = pl.pallas_call(
        scale_kernel,
        out_shape=(
            jax.ShapeDtypeStruct((near_null.shape[0], slots, rows), jnp.bfloat16),
            jax.ShapeDtypeStruct(near_null.shape, jnp.bfloat16),
            jax.ShapeDtypeStruct((1, 1), f32),
        ),
        in_specs=[vmem, vmem, vmem],
        out_specs=(vmem, vmem, vmem),
        compiler_params=pltpu.CompilerParams(vmem_limit_bytes=16777216),
        name="scale",
    )(raw, tentative, rho)
    return (prolong_off.transpose(1, 0, 2), prolong_self, rho.reshape(()))


def solution(mesh):
    placed = (
        P(None, ("slab", "sub")),
        P(("slab", "sub")),
        P(None, ("slab", "sub")),
        P(None, None, ("slab", "sub")),
        P(None, ("slab", "sub")),
        P(None, ("slab", "sub")),
        P(None, ("slab", "sub")),
    )
    return jax.shard_map(
        functools.partial(body, mesh.shape["slab"], mesh.shape["sub"]),
        mesh=mesh,
        in_specs=placed,
        out_specs=(P(None, None, ("slab", "sub")), P(None, ("slab", "sub")), P()),
        check_vma=False,
    )
```

```python
import functools

import jax
import jax.numpy as jnp
from jax import lax
from jax.experimental import pallas as pl
from jax.experimental.pallas import tpu as pltpu
from jax.sharding import PartitionSpec as P

ITERS = 8
OMEGA = 4.0 / 3.0
LANES = 128
MESH = pl.DeviceIdType.MESH
LOAD_ORDER = [0, 1, 4, 5, 2, 3]
DEPTH = 2
BLOCKS = ITERS // DEPTH
WAYS = [(0, 1), (0, -1), (1, 0), (-1, 0)]
FAR = [(-1, -1), (-1, 1), (1, -1), (1, 1), (-2, 0), (2, 0), (0, -2), (0, 2)]
CIRCLE = WAYS + FAR
ORDER = list(range(len(WAYS), len(CIRCLE))) + list(range(len(WAYS)))


def lane_gather(table, lanes):
    return jnp.take_along_axis(table, lanes, axis=1, mode="promise_in_bounds")


def tile(number):
    return pl.ds(number * LANES, LANES)


def pick(tables, index, first):
    high = index >> 7
    low = index & (LANES - 1)
    out = jnp.zeros(index.shape, jnp.float32)
    for step, table in enumerate(tables):
        out = jnp.where(high == first + step, lane_gather(table, low), out)
    return out


def invert_rows(entries):
    cofactor = [
        entries[4] * entries[8] - entries[5] * entries[7],
        entries[5] * entries[6] - entries[3] * entries[8],
        entries[3] * entries[7] - entries[4] * entries[6],
        entries[2] * entries[7] - entries[1] * entries[8],
        entries[0] * entries[8] - entries[2] * entries[6],
        entries[1] * entries[6] - entries[0] * entries[7],
        entries[1] * entries[5] - entries[2] * entries[4],
        entries[2] * entries[3] - entries[0] * entries[5],
        entries[0] * entries[4] - entries[1] * entries[3],
    ]
    determinant = entries[0] * cofactor[0] + entries[1] * cofactor[1] + entries[2] * cofactor[2]
    return [
        cofactor[column * 3 + row] / determinant for row in range(3) for column in range(3)
    ]


def unit_places(slots, tiles):
    units = []
    for k in range(0, slots - 7, 8):
        for j in range(tiles):
            units.append([(0, k, 8, j)])
    rest = slots % 8
    if rest:
        share = 8 // rest
        for j in range(0, tiles, share):
            units.append(
                [
                    (rest * i, slots - rest, rest, j + i)
                    for i in range(min(share, tiles - j))
                ]
            )
    return units


def scale_kernel(raw_ref, tent_ref, rho_ref, off_ref, self_ref, out_rho_ref):
    slots, rows = off_ref.shape[1:]
    out_rho_ref[...] = rho_ref[0:1, 0:1]
    inverse = OMEGA / rho_ref[...]
    factor = -inverse
    places = unit_places(slots, rows // LANES)
    for j in range(rows // LANES):
        for entry in range(off_ref.shape[0]):
            parts = [
                (raw_ref[entry, u] * factor)[at : at + count]
                for u in range(len(places))
                for at, k, count, tile_number in places[u]
                if tile_number == j
            ]
            off_ref[entry, :, tile(j)] = jnp.concatenate(parts, axis=0).astype(off_ref.dtype)
    self_ref[...] = ((1.0 - inverse[0:1, 0:1]) * tent_ref[...]).astype(self_ref.dtype)


def kernel(
    n_slab, n_sub,
    near_hbm, agg_hbm, diag_hbm, off_hbm, cols_hbm, sends_hbm, start_hbm,
    raw_ref, tent_ref, rho_ref,
    near_ref, agg_ref, diag_ref, cols_ref, sends_ref, start_ref, off_v, cols_u, mats, rest_m, dinv, text, hist, sidx,
    sendw, recvw, sendu, recvu, mine, minecol, sendg, recvg, gcol, sendt, recvt, stat, stats,
    ss_sem, rs_sem,
):
    a = lax.axis_index("slab")
    b = lax.axis_index("sub")
    devices = n_slab * n_sub

    def power(
        off_sem, sendw_sem, recvw_sem, sendu_sem, recvu_sem, sendg_sem, recvg_sem, sendt_sem, recvt_sem
    ):
        slots, rows = cols_ref.shape
        half = sends_ref.shape[1]
        tiles = rows // LANES
        units = unit_places(slots, tiles)
        groups = -(-slots // 8)
        gunits, planes = sendg.shape[1:3]
        modes = near_ref.shape[0] // 3
        sizes_of = rows // 8
        barrier = pltpu.get_barrier_semaphore()
        def present(x, y):
            return (a + x >= 0) & (a + x < n_slab) & (b + y >= 0) & (b + y < n_sub)

        def greet(x, y):
            pl.semaphore_signal(
                barrier, inc=1, device_id={"slab": a + x, "sub": b + y}, device_id_type=MESH
            )

        def greet_any(step, unused):
            target = lax.rem(a * n_sub + b + step, n_slab * n_sub)
            greet(lax.div(target, n_sub) - a, lax.rem(target, n_sub) - b)
            return unused

        near = n_slab - 1 + n_sub - 1 <= ITERS + 2
        if near:
            for place in ORDER:
                x, y = CIRCLE[place]
                pl.when(present(x, y))(functools.partial(greet, x, y))
            greeters = sum(present(x, y).astype(jnp.int32) for x, y in CIRCLE)
        else:
            lax.fori_loop(1, n_slab * n_sub, greet_any, 0)
            greeters = n_slab * n_sub - 1

        loads = [
            pltpu.make_async_copy(source, target, off_sem.at[number])
            for number, (source, target) in enumerate(
                (
                    (start_hbm, start_ref),
                    (sends_hbm, sends_ref),
                    (agg_hbm, agg_ref),
                    (near_hbm, near_ref),
                    (diag_hbm, diag_ref),
                    (cols_hbm, cols_ref),
                )
            )
        ]
        deep = [min(8, -(-(slots - 16 * v) // 2)) for v in range(gunits)]
        cuts = [(16 * v, min(16, slots - 16 * v)) for v in range(gunits)]
        loads += [
            pltpu.make_async_copy(
                off_hbm.at[:, pl.ds(k, count)], off_v.at[:, pl.ds(k, count)], off_sem.at[len(loads) + v]
            )
            for v, (k, count) in enumerate(cuts)
        ]
        for number in LOAD_ORDER + list(range(len(LOAD_ORDER), len(loads))):
            loads[number].start()

        for way in range(len(WAYS)):
            for v in range(gunits):
                if deep[v] < 8:
                    recvg[way, v, :, deep[v] : 8, :] = jnp.zeros((planes, 8 - deep[v], LANES), jnp.float32)

        def clear(place):
            cleared = [recvw.at[:, place]]
            if place < len(WAYS):
                cleared += [recvu.at[:, place], recvg.at[place], recvt.at[place]]
            for ref in cleared:
                ref[...] = jnp.zeros(ref.shape, jnp.float32)

        for place, (x, y) in enumerate(CIRCLE):
            pl.when(jnp.logical_not(present(-x, -y)))(functools.partial(clear, place))

        def remote(source, target, sent, came, place):
            x, y = CIRCLE[place]
            return pltpu.make_async_remote_copy(
                src_ref=source, dst_ref=target, send_sem=sent, recv_sem=came,
                device_id={"slab": a + x, "sub": b + y}, device_id_type=MESH,
            )

        def w_copy(turn, place):
            x, y = CIRCLE[place]
            part = pl.ds(4, 4) if y == 0 else pl.ds(0, 4) if x == 0 else pl.ds(0, 8)
            return remote(
                sendw.at[turn, part], recvw.at[turn, place, part],
                sendw_sem.at[place], recvw_sem.at[lax.rem(turn, 2), place], place,
            )

        def u_copy(turn, way):
            part = pl.ds(4 * (way // 2), 4)
            return remote(
                sendu.at[turn, part], recvu.at[turn, way, part],
                sendu_sem.at[way], recvu_sem.at[lax.rem(turn, 2), way], way,
            )

        def g_copy(v, way):
            part = pl.ds(0, deep[v])
            return remote(
                sendg.at[way, v, :, part], recvg.at[way, v, :, part],
                sendg_sem.at[way, v], recvg_sem.at[way, v], way,
            )

        def t_copy(way):
            return remote(sendt.at[way // 2], recvt.at[way], sendt_sem.at[way], recvt_sem.at[way], way)

        def each_target(make, places, act):
            for place in places:
                x, y = CIRCLE[place]
                pl.when(present(x, y))(functools.partial(lambda place: act(make(place)), place))

        def each_source(make, places):
            for place in places:
                x, y = CIRCLE[place]
                pl.when(present(-x, -y))(functools.partial(lambda place: make(place).wait_recv(), place))

        def begin_copy(copy):
            copy.start()

        def settle(copy):
            copy.wait_send()

        ways = range(len(WAYS))
        far = range(len(WAYS), len(CIRCLE))
        left = lax.broadcasted_iota(jnp.int32, (8, LANES), 1) < half

        hist[...] = jnp.zeros_like(hist)
        loads[0].wait()
        loads[1].wait()
        hist[0, 0:3, :] = start_ref[...]
        for pair in range(2):
            sidx[pair] = jnp.broadcast_to(
                jnp.concatenate(
                    [sends_ref[2 * pair : 2 * pair + 1, :], sends_ref[2 * pair + 1 : 2 * pair + 2, :]],
                    axis=1,
                ),
                (8, LANES),
            )

        def listed(step):
            tables = [hist[step, :, tile(j)] for j in range(tiles)]
            picked = [pick(tables, sidx[pair], 0) for pair in range(2)]
            return jnp.concatenate([picked[0][0:4], picked[1][0:4]], axis=0)

        sendw[...] = jnp.zeros_like(sendw)
        sendu[...] = jnp.zeros_like(sendu)
        sendw[0] = listed(0)

        loads[4].wait()
        loads[5].wait()
        inverse = invert_rows([diag_ref[p : p + 1, :] for p in range(9)])
        for p in range(9):
            dinv[p : p + 1, :] = inverse[p]
        rest_m[...] = jnp.zeros_like(rest_m)
        for u, places in enumerate(units):
            if len(places) * places[0][2] < 8:
                cols_u[u] = jnp.zeros((8, LANES), jnp.int32)
            for at, k, count, j in places:
                cols_u[u, at : at + count, :] = cols_ref[k : k + count, tile(j)]
                if count < 8:
                    rest_m[planes - 1, j, 0:count, :] = cols_ref[k : k + count, tile(j)].astype(jnp.float32)

        def source(q, group, j):
            if 8 * (group + 1) > slots:
                return rest_m[q, j]
            u = group * tiles + j
            return cols_u[u].astype(jnp.float32) if q == planes - 1 else mats[u, q]

        def chosen(q, group, pair):
            if group >= groups:
                return jnp.zeros((8, LANES), jnp.float32)
            return pick([source(q, group, j) for j in range(tiles)], sidx[pair], 0)

        for v, (cut, length) in enumerate(cuts):
            loads[6 + v].wait()
            for u, places in enumerate(units):
                if not cut <= places[0][1] < cut + length:
                    continue
                if len(places) * places[0][2] < 8:
                    mats[u] = jnp.zeros(mats.shape[1:], jnp.float32)
                for at, k, count, j in places:
                    block = [off_v[p, k : k + count, tile(j)] for p in range(9)]
                    for r in range(3):
                        scale = [
                            jnp.broadcast_to(dinv[3 * r + q : 3 * r + q + 1, tile(j)], (count, LANES))
                            for q in range(3)
                        ]
                        for c in range(3):
                            entry = scale[0] * block[c] + scale[1] * block[3 + c] + scale[2] * block[6 + c]
                            mats[u, 3 * r + c, at : at + count, :] = entry
                            if count < 8:
                                rest_m[3 * r + c, j, 0:count, :] = entry
        def pack_rows(v, pair):
            count = deep[v]
            for q in range(planes):
                low = chosen(q, 2 * v, pair)
                high = chosen(q, 2 * v + 1, pair)
                for group, listing in ((2 * v, low), (2 * v + 1, high)):
                    if group < groups and q < planes - 1:
                        mine[pair, group, q] = listing
                    elif group < groups:
                        minecol[pair, group] = listing.astype(jnp.int32)
                if count < 8:
                    high = jnp.concatenate([low[count:8], high[0:count]], axis=0)
                sendg[2 * pair, v, q] = jnp.where(left, low, pltpu.roll(high, half, 1))
                sendg[2 * pair + 1, v, q] = jnp.where(left, pltpu.roll(low, half, 1), high)

        for number, (v, pair) in enumerate([(v, pair) for v in range(gunits) for pair in (0, 1)]):
            pack_rows(v, pair)
            if number == 0:
                pl.semaphore_wait(barrier, greeters)
                each_target(functools.partial(w_copy, 0), ORDER, begin_copy)
            each_target(functools.partial(g_copy, v), (2 * pair, 2 * pair + 1), begin_copy)

        def tentative():
            loads[2].wait()
            loads[3].wait()
            agg = agg_ref[...]
            member = (
                jnp.broadcast_to(agg, (sizes_of, rows)) == lax.broadcasted_iota(jnp.int32, (sizes_of, rows), 0)
            ).astype(jnp.float32)
            counts = jnp.sum(member, axis=1, keepdims=True)
            sizes = jnp.sum(member * counts, axis=0, keepdims=True)
            tent_ref[...] = near_ref[...] * lax.rsqrt(sizes)
            text[...] = jnp.zeros_like(text)
            for c in range(3):
                text[8 * c : 8 * c + modes, 0:rows] = tent_ref[modes * c : modes * (c + 1), :]
            for pair in range(2):
                for c in range(3):
                    sendt[pair, 8 * c : 8 * c + 8, :] = pick(
                        [text[8 * c : 8 * c + 8, tile(j)] for j in range(tiles)], sidx[pair], 0
                    )
            each_target(t_copy, ways, begin_copy)

        per = -(-len(units) // (BLOCKS - 1))

        def spread(row):
            return jnp.broadcast_to(row, (8, LANES))

        def unit_products(u, unused):
            index = cols_u[u]
            for m in range(modes):
                picked = [
                    pick(
                        [
                            spread(text[8 * c + m : 8 * c + m + 1, tile(i)])
                            for i in range(tiles + 2)
                        ],
                        index,
                        0,
                    )
                    for c in range(3)
                ]
                for r in range(3):
                    raw_ref[modes * r + m, u] = (
                        mats[u, 3 * r] * picked[0]
                        + mats[u, 3 * r + 1] * picked[1]
                        + mats[u, 3 * r + 2] * picked[2]
                    )
            return unused

        def contribute(tables, first, u):
            index = cols_u[u]
            picked = [pick(tables[c], index, first) for c in range(3)]
            return [sum(mats[u, 3 * r + c] * picked[c] for c in range(3)) for r in range(3)]

        def contribute_near(tables, first, way):
            total = [None] * 3
            for v in range(gunits):
                index = gcol[way, v]
                picked = [pick(tables[c], index, first) for c in range(3)]
                for r in range(3):
                    term = sum(recvg[way, v, 3 * r + c] * picked[c] for c in range(3))
                    total[r] = term if total[r] is None else total[r] + term
            return total

        def contribute_mine(tables, first):
            total = [[None] * 3 for pair in range(2)]
            for pair in range(2):
                for group in range(groups):
                    index = minecol[pair, group]
                    picked = [pick(tables[c], index, first) for c in range(3)]
                    for r in range(3):
                        term = sum(mine[pair, group, 3 * r + c] * picked[c] for c in range(3))
                        total[pair][r] = term if group == 0 else total[pair][r] + term
            return total

        def own_tables(step):
            return [[spread(hist[step, c : c + 1, tile(i)]) for i in range(tiles)] for c in range(3)]

        def by_tile(terms):
            whole = [[None] * tiles for r in range(3)]
            for r in range(3):
                for u, places in enumerate(units):
                    if len(places) == 1 and places[0][2] == 8:
                        j = places[0][3]
                        old = whole[r][j]
                        whole[r][j] = terms[u][r] if old is None else old + terms[u][r]
                for j in range(tiles):
                    old = whole[r][j]
                    whole[r][j] = 0.0 if old is None else jnp.sum(old, axis=0, keepdims=True)
                for u, places in enumerate(units):
                    if not (len(places) == 1 and places[0][2] == 8):
                        for at, k, count, j in places:
                            whole[r][j] = whole[r][j] + jnp.sum(
                                terms[u][r][at : at + count], axis=0, keepdims=True
                            )
            return whole

        def own_part(step):
            tables = own_tables(step)
            inner = by_tile([contribute(tables, 0, u) for u in range(len(units))])
            for r in range(3):
                for j in range(tiles):
                    hist[step + 1, r : r + 1, tile(j)] = hist[step, r : r + 1, tile(j)] + inner[r][j]

        def ghost_part(step, tables):
            outer = by_tile([contribute(tables, tiles, u) for u in range(len(units))])
            for r in range(3):
                for j in range(tiles):
                    hist[step + 1, r : r + 1, tile(j)] = hist[step + 1, r : r + 1, tile(j)] + outer[r][j]

        def halves(first, second, pair):
            part = pl.ds(4 * pair, 4)
            both = jnp.where(left[0:4], first[part, :], second[part, :])
            return [both[c : c + 1] for c in range(3)]

        def iterate(turn, last):
            step = DEPTH * turn
            inner = contribute_mine(own_tables(step), 0)
            for pair in range(2):
                for r in range(3):
                    at = pl.ds(4 * pair + r, 1)
                    sendu[turn, at, :] = sendw[turn, at, :] + jnp.sum(inner[pair][r], axis=0, keepdims=True)
            each_target(functools.partial(u_copy, turn), ways, begin_copy)
            own_part(step)
            pl.when(turn == 0)(tentative)

            @pl.when(turn == 1)
            def _():
                each_source(t_copy, ways)
                for pair in range(2):
                    for c in range(3):
                        text[8 * c : 8 * c + 8, tile(tiles + pair)] = jnp.where(
                            left,
                            recvt[2 * pair, 8 * c : 8 * c + 8, :],
                            recvt[2 * pair + 1, 8 * c : 8 * c + 8, :],
                        )

            lax.fori_loop(
                jnp.clip((turn - 1) * per, 0, len(units)), jnp.clip(turn * per, 0, len(units)), unit_products, 0
            )
            each_target(functools.partial(w_copy, turn), ORDER, settle)
            each_target(functools.partial(u_copy, turn), ways, settle)
            each_source(functools.partial(w_copy, turn), ways)
            merged = [halves(recvw.at[turn, 2 * pair], recvw.at[turn, 2 * pair + 1], pair) for pair in range(2)]
            ghost_part(step, [[spread(merged[pair][c]) for pair in range(2)] for c in range(3)])
            if last:
                own_part(step + 1)
                stat[1] = squares(step + 1)
            else:
                kept = listed(step + 1)
                inner = contribute_mine(own_tables(step + 1), 0)

            @pl.when(turn == 0)
            def _():
                for v in range(gunits):
                    each_source(functools.partial(g_copy, v), ways)
                for way in ways:
                    for v in range(gunits):
                        gcol[way, v] = recvg[way, v, planes - 1].astype(jnp.int32)

            each_source(functools.partial(w_copy, turn), far)

            def packed(way, other):
                x, y = (WAYS[way][axis] + WAYS[other][axis] for axis in range(2))
                return sendw.at[turn] if (x, y) == (0, 0) else recvw.at[turn, CIRCLE.index((x, y))]

            total = []
            for way in ways:
                rows_of = [
                    halves(packed(way, 2 * pair), packed(way, 2 * pair + 1), pair) for pair in range(2)
                ]
                total.append(
                    contribute_near(
                        [[spread(rows_of[pair][c]) for pair in range(2)] for c in range(3)], tiles, way
                    )
                )
            each_source(functools.partial(u_copy, turn), ways)
            base = [halves(recvu.at[turn, 2 * pair], recvu.at[turn, 2 * pair + 1], pair) for pair in range(2)]
            later = [[], [], []]
            for r in range(3):
                for pair in range(2):
                    first, second = total[2 * pair][r], total[2 * pair + 1][r]
                    both = jnp.where(left, first, second) + pltpu.roll(
                        jnp.where(left, second, first), half, 1
                    )
                    later[r].append(spread(base[pair][r] + jnp.sum(both, axis=0, keepdims=True)))
            if last:
                ghost_part(step + 1, later)
                return
            outer = contribute_mine(later, tiles)
            for pair in range(2):
                for r in range(3):
                    row = 4 * pair + r
                    sendw[turn + 1, row : row + 1, :] = kept[row : row + 1] + jnp.sum(
                        inner[pair][r] + outer[pair][r], axis=0, keepdims=True
                    )
            each_target(functools.partial(w_copy, turn + 1), ORDER, begin_copy)
            own_part(step + 1)
            ghost_part(step + 1, later)

        def squares(step):
            return jnp.sum(
                sum(hist[step, :, tile(j)] * hist[step, :, tile(j)] for j in range(tiles)),
                axis=0, keepdims=True,
            )

        def advance(turn, unused):
            iterate(turn, False)
            return unused

        lax.fori_loop(0, BLOCKS - 1, advance, 0)
        iterate(BLOCKS - 1, True)

        latest, previous = squares(ITERS), stat[1]
        stat[0] = jnp.where(left[0:1], latest, previous) + pltpu.roll(
            jnp.where(left[0:1], previous, latest), half, 1
        )
        me = a * n_sub + b

        def begin(step, unused):
            target = lax.rem(me + jnp.where(2 * a < n_slab, devices - step, step), devices)
            pltpu.make_async_remote_copy(
                src_ref=stat.at[0], dst_ref=stats.at[me], send_sem=ss_sem, recv_sem=rs_sem,
                device_id={"slab": lax.div(target, n_sub), "sub": lax.rem(target, n_sub)},
                device_id_type=MESH,
            ).start()
            return unused

        lax.fori_loop(1, devices, begin, 0, unroll=devices <= 64)
        stats[me] = stat[0]
        for v in range(gunits):
            each_target(functools.partial(g_copy, v), ways, settle)
        each_target(t_copy, ways, settle)

    dma = pltpu.SemaphoreType.DMA
    ways = len(WAYS)
    pl.run_scoped(
        power,
        dma((6 + sendg.shape[1],)),
        dma((len(CIRCLE),)),
        dma((2, len(CIRCLE))),
        dma((ways,)),
        dma((2, ways)),
        dma((ways, sendg.shape[1])),
        dma((ways, sendg.shape[1])),
        dma((ways,)),
        dma((ways,)),
    )
    others = stats.at[pl.ds(0, devices - 1)]
    everything = pltpu.make_async_remote_copy(
        src_ref=others, dst_ref=others, send_sem=ss_sem, recv_sem=rs_sem,
        device_id={"slab": n_slab - 1 - a, "sub": n_sub - 1 - b}, device_id_type=MESH,
    )
    everything.wait_recv()
    whole = jnp.sum(stats[...], axis=0)
    first = lax.broadcasted_iota(jnp.int32, (1, LANES), 1) < sends_ref.shape[1]
    latest = jnp.sum(jnp.where(first, whole, 0.0), axis=1, keepdims=True)
    previous = jnp.sum(jnp.where(first, 0.0, whole), axis=1, keepdims=True)
    rho_ref[...] = jnp.broadcast_to(jnp.sqrt(latest / (previous + 1e-05)), rho_ref.shape)

    everything.wait_send()


def body(n_slab, n_sub, near_null, aggregates, diag_block, off_blocks, columns, sends, start_vector):
    slots, nine, rows = off_blocks.shape
    wide = rows + 2 * LANES
    count = len(unit_places(slots, rows // LANES))
    gunits = -(-slots // 16)
    f32 = jnp.float32
    vmem = pl.BlockSpec(memory_space=pltpu.VMEM)
    dma = pltpu.SemaphoreType.DMA
    raw, tentative, rho = pl.pallas_call(
        functools.partial(kernel, n_slab, n_sub),
        out_shape=(
            pltpu.VMEM((near_null.shape[0], count, 8, LANES), f32),
            pltpu.VMEM(near_null.shape, f32),
            pltpu.VMEM((8, LANES), f32),
        ),
        in_specs=[pl.BlockSpec(memory_space=pltpu.HBM)] * 7,
        out_specs=(vmem, vmem, vmem),
        scratch_shapes=[
            pltpu.VMEM(near_null.shape, f32),
            pltpu.VMEM((1, rows), jnp.int32),
            pltpu.VMEM(diag_block.shape, f32),
            pltpu.VMEM(columns.shape, jnp.int32),
            pltpu.VMEM(sends.shape, jnp.int32),
            pltpu.VMEM(start_vector.shape, f32),
            pltpu.VMEM((nine, slots, rows), f32),
            pltpu.VMEM((count, 8, LANES), jnp.int32),
            pltpu.VMEM((count, nine, 8, LANES), f32),
            pltpu.VMEM((nine + 1, rows // LANES, 8, LANES), f32),
            pltpu.VMEM((16, rows), f32),
            pltpu.VMEM((24, wide), f32),
            pltpu.VMEM((ITERS + 1, 8, rows), f32),
            pltpu.VMEM((2, 8, LANES), jnp.int32),
            pltpu.VMEM((BLOCKS, 8, LANES), f32),
            pltpu.VMEM((BLOCKS, len(CIRCLE), 8, LANES), f32),
            pltpu.VMEM((BLOCKS, 8, LANES), f32),
            pltpu.VMEM((BLOCKS, len(WAYS), 8, LANES), f32),
            pltpu.VMEM((2, -(-slots // 8), nine, 8, LANES), f32),
            pltpu.VMEM((2, -(-slots // 8), 8, LANES), jnp.int32),
            pltpu.VMEM((len(WAYS), gunits, nine + 1, 8, LANES), f32),
            pltpu.VMEM((len(WAYS), gunits, nine + 1, 8, LANES), f32),
            pltpu.VMEM((len(WAYS), gunits, 8, LANES), jnp.int32),
            pltpu.VMEM((2, 24, LANES), f32),
            pltpu.VMEM((4, 24, LANES), f32),
            pltpu.VMEM((2, 1, LANES), f32),
            pltpu.VMEM((n_slab * n_sub, 1, LANES), f32),
            dma,
            dma,
        ],
        compiler_params=pltpu.CompilerParams(collective_id=0, has_side_effects=True, vmem_limit_bytes=16777216),
        name="smooth",
    )(
        *[
            pltpu.with_memory_space_constraint(x, pltpu.HBM)
            for x in (
                near_null, aggregates.reshape(1, rows), diag_block, off_blocks.transpose(1, 0, 2),
                columns, sends, start_vector,
            )
        ]
    )
    prolong_off, prolong_self, rho = pl.pallas_call(
        scale_kernel,
        out_shape=(
            jax.ShapeDtypeStruct((near_null.shape[0], slots, rows), jnp.bfloat16),
            jax.ShapeDtypeStruct(near_null.shape, jnp.bfloat16),
            jax.ShapeDtypeStruct((1, 1), f32),
        ),
        in_specs=[vmem, vmem, vmem],
        out_specs=(vmem, vmem, vmem),
        compiler_params=pltpu.CompilerParams(vmem_limit_bytes=16777216),
        name="scale",
    )(raw, tentative, rho)
    return (prolong_off.transpose(1, 0, 2), prolong_self, rho.reshape(()))


def solution(mesh):
    placed = (
        P(None, ("slab", "sub")),
        P(("slab", "sub")),
        P(None, ("slab", "sub")),
        P(None, None, ("slab", "sub")),
        P(None, ("slab", "sub")),
        P(None, ("slab", "sub")),
        P(None, ("slab", "sub")),
    )
    return jax.shard_map(
        functools.partial(body, mesh.shape["slab"], mesh.shape["sub"]),
        mesh=mesh,
        in_specs=placed,
        out_specs=(P(None, None, ("slab", "sub")), P(None, ("slab", "sub")), P()),
        check_vma=False,
    )
```
